32 devices in a mesh: docs: 8 (over z, x), rep: 4 (over y, core).
Axes of the slice: x: 2, y: 2, z: 4, core: 2. Of those that a mesh axis runs over, the one named last changes fastest.
Arguments:
- embeddings: bfloat16 [32768, 4096], P(('docs', 'rep')), may hold values from -6 to 6
- pca_basis: bfloat16 [4096, 256], replicated, may hold values from -0.09375 to 0.09375
- cluster: int32 [32768, 1], P(('docs', 'rep')), may hold values from 0 to 31; in each aligned block of 1024 rows (0 to 1023, 1024 to 2047, ...) at most 64 rows name the same one
- doc_index: int32 [32768], P(('docs', 'rep')), may hold values from 0 to 32767, each once
Outputs:
- nearest_sim: float32 [32768], P(('docs', 'rep'))
The draws below stay inside these ranges and needn't reach their ends.
Inputs may be any that keep to these rules, and one draw needn't show every extreme that they name: In each device's block of 1024 rows no cluster is named by more than 64 rows, a bound that some block reaches. `doc_index`: each document number appears once.
All inputs are finite; a program needn't handle non-finite values.
Results may differ from the reference program's by a relative error of at most 0.0014.
Values may be sent and summed in bfloat16 or wider, within the bound.
No kernel may reach another device: no remote copies, remote signals or barrier semaphores. Data moves between devices by JAX's collectives and lax.ppermute only.
A program may use at most 64 MiB of HBM per device.

```python
import math
import jax
import jax.numpy as jnp
import numpy as np
from jax import lax

E = 4096
P_SIZE = 256
DOC_DEV = 1024
CLUSTERS = 32
MOST = 64
DOCS = 32768
CAP = 2048


def levels(own_key, extent, cuts, least, largest):
    loudness, own = 1.0, jax.random.fold_in(own_key, 6)
    for position, blocks in cuts:
        heights = jnp.exp(jax.random.uniform(jax.random.fold_in(own, position), (blocks,), jnp.float32, least / len(cuts), largest / len(cuts)))
        loudness = loudness * jnp.repeat(heights, extent[position] // blocks).reshape([-1 if axis == position else 1 for axis in range(len(extent))])
    return loudness


def routed_block(own_key, own, number, rows, number_of, top, most, lean):
    sequence = jax.random.permutation(own_key, number_of)
    crowded, ordinary = shares(number_of, rows * top, most, lean, True), shares(number_of, rows * top, most, lean, False)
    places = jnp.arange(number_of)

    def named(sizes, turn):
        used = int((sizes > 0).sum())
        fixed = max(1, used // 4)
        passed = fixed + (places - fixed + turn * (used - fixed)) % max(1, number_of - fixed)
        return jnp.zeros((number_of,), jnp.int32).at[sequence[jnp.where(places < fixed, places, passed)]].set(jnp.asarray(sizes, jnp.int32))

    sizes = jnp.where(number % 4 == 0, named(crowded, number // 4), named(ordinary, number - number // 4 - 1))
    mixed = jax.random.permutation(jax.random.fold_in(own, 3), number_of)
    donor, sink = mixed[0:number_of // 2 * 2:2], mixed[1:number_of // 2 * 2:2]
    room = jnp.minimum(sizes[donor] - 1, most - sizes[sink]) // 2
    room = jnp.where((donor == sequence[0]) | (sink == sequence[0]) | (sizes[sink] == 0), 0, jnp.maximum(room, 0))
    passed = jax.random.randint(jax.random.fold_in(own, 4), (number_of // 2,), 0, 1 << 20) % (room + 1)
    sizes = sizes.at[donor].add(-passed).at[sink].add(passed)
    labels = jnp.searchsorted(jnp.cumsum(sizes), jnp.arange(rows * top), side="right").astype(jnp.int32)
    table = labels.reshape(top, rows).T
    table = table[jax.random.permutation(jax.random.fold_in(own, 1), rows)]
    turn = jax.random.randint(jax.random.fold_in(own, 2), (rows, 1), 0, top)
    return jnp.take_along_axis(table, (jnp.arange(top)[None, :] + turn) % top, axis=1)


def shares(count, total, most, slope, full):
    weights = [(1 << 20) // math.isqrt(standing ** slope) + 1 for standing in range(1, count + 1)]
    largest = most if full else min(most, max(-(-total // count), total * weights[0] // sum(weights)))
    least = 1 if total - largest >= count - 1 else 0
    given, spare = [largest] + [least] * (count - 1), total - largest - least * (count - 1)
    while spare > 0:
        free = [i for i in range(1, count) if given[i] < largest] or [i for i in range(1, count) if given[i] < most]
        pool, left = sum([weights[i] for i in free]), spare
        for i in free:
            extra = min(most - given[i], max(1, left * weights[i] // pool), spare)
            given[i] = given[i] + extra
            spare = spare - extra
    return np.array(given)


def scatter_about(stream_key, extent, width, bound, shards=(), held_as=jnp.bfloat16):
    array = jax.random.normal(stream_key, extent, jnp.float32) * width
    if len(shards) > 0:
        array = levels(stream_key, extent, shards, -0.22, 0.18) * array
    return jnp.clip(array, min=-bound, max=bound).astype(held_as)


def setup_inputs(seed: int = 0) -> dict:
    seeds = jax.random.split(jax.random.key(seed), 5)
    embeddings = scatter_about(seeds[0], (DOCS, E), 1.0, 6.0, ((0, 32),))
    pca_basis = scatter_about(seeds[1], (E, P_SIZE), E ** -0.5, 0.09375)
    cluster_keys = jax.random.split(jax.random.fold_in(seeds[2], 1), DOCS // DOC_DEV)
    cluster_turns = jax.random.permutation(jax.random.fold_in(seeds[2], 3), DOCS // DOC_DEV)
    cluster = jax.vmap(lambda own, number: routed_block(jax.random.fold_in(seeds[2], 2), own, number, DOC_DEV, CLUSTERS, 1, MOST, 2))(cluster_keys, cluster_turns).reshape((DOCS, 1))
    doc_index = jax.random.permutation(seeds[3], DOCS).astype(jnp.int32)
    return dict(embeddings=embeddings, pca_basis=pca_basis, cluster=cluster, doc_index=doc_index)


def project_rows(embeddings, pca_basis):
    blocks = embeddings.reshape(-1, DOC_DEV, embeddings.shape[1])
    basis_wide = pca_basis.astype(jnp.float32)

    def single(block):
        return jnp.dot(block.astype(jnp.float32), basis_wide, precision=lax.Precision.HIGHEST)
    projected = lax.map(single, blocks).reshape(-1, pca_basis.shape[1])
    scaled = projected * lax.rsqrt(lax.optimization_barrier(jnp.sum(projected * projected, axis=1, keepdims=True)) + 1e-06)
    return scaled.astype(jnp.bfloat16)

def reference(embeddings, pca_basis, cluster, doc_index):
    unit_rows = project_rows(embeddings, pca_basis)
    cluster_id = cluster[:, 0].astype(jnp.int32)
    order = jnp.argsort(cluster_id * DOCS + doc_index).astype(jnp.int32)
    sorted_rows = unit_rows[order]
    sorted_ids = cluster_id[order]
    counts = jnp.zeros((CLUSTERS,), jnp.int32).at[cluster_id].add(1)
    starts = (jnp.cumsum(counts) - counts).astype(jnp.int32)
    padded = jnp.concatenate([sorted_rows, jnp.zeros((CAP, sorted_rows.shape[1]), sorted_rows.dtype)], axis=0)
    places = jnp.arange(CAP, dtype=jnp.int32)

    def per_cluster(inputs):
        begin, amount = inputs
        members = lax.dynamic_slice_in_dim(padded, begin, CAP, 0)
        scores = jnp.dot(members, members.T, preferred_element_type=jnp.float32)
        allowed = (places[None, :] < places[:, None]) & (places[None, :] < amount)
        return lax.optimization_barrier(jnp.max(jnp.where(allowed, scores, -1.0), axis=1))
    results = lax.map(per_cluster, (starts, counts))
    offsets = jnp.arange(DOCS, dtype=jnp.int32) - starts[sorted_ids]
    values = results[sorted_ids, offsets]
    return jnp.zeros_like(values).at[order].set(values)
```

```python
import jax
import jax.numpy as jnp
from jax import lax
from jax.experimental import pallas as pl
from jax.experimental.pallas import tpu as pltpu
from jax.sharding import PartitionSpec as P

CL_DEV = 4
AXES = ("docs", "rep")
LANES = 128
EXTRA = 8
CHUNKS = 8
BASE = 256


def nt_dot(a, b):
    return lax.dot_general(a, b, (((1,), (1,)), ((), ())), preferred_element_type=jnp.float32)


def project_and_pack(
    cluster_ref, index_ref, emb_hbm, basis_hbm, send_ref, lane_ref,
    emb, basis, rows, place, emb_sem, basis_sem, *, depth, clusters, total,
):
    n_rows, width = emb.shape
    features = basis.shape[1]
    step = n_rows // CHUNKS

    def emb_copy(k):
        part = pl.ds(k * step, step)
        return pltpu.make_async_copy(emb_hbm.at[part], emb.at[part], emb_sem.at[k])

    basis_copy = pltpu.make_async_copy(basis_hbm, basis, basis_sem)
    basis_copy.start()
    for k in range(CHUNKS):
        emb_copy(k).start()

    cluster = cluster_ref[...]
    blocks = n_rows // LANES
    cluster_iota = lax.broadcasted_iota(jnp.int32, (clusters, n_rows), 0)
    member = cluster_iota == cluster
    member_f = member.astype(jnp.float32)
    stacked = jnp.concatenate(
        [member_f[:, b * LANES:(b + 1) * LANES] for b in range(blocks)], axis=0
    ).astype(jnp.bfloat16)
    row_id = lax.broadcasted_iota(jnp.int32, (LANES, 2 * LANES), 0)
    col_id = lax.broadcasted_iota(jnp.int32, (LANES, 2 * LANES), 1)
    earlier = ((row_id < col_id) | (col_id >= LANES)).astype(jnp.float32).astype(jnp.bfloat16)
    prefix = jnp.dot(stacked, earlier, preferred_element_type=jnp.float32)
    carry = jnp.zeros((clusters, LANES), jnp.float32)
    ranks = []
    for b in range(blocks):
        part = prefix[b * clusters:(b + 1) * clusters]
        mine = member_f[:, b * LANES:(b + 1) * LANES]
        ranks.append(jnp.sum(mine * (part[:, :LANES] + carry), axis=0, keepdims=True))
        carry = carry + part[:, LANES:]
    rank = jnp.concatenate(ranks, axis=1).astype(jnp.int32)
    me = lax.axis_index("docs") * lax.axis_size("rep") + lax.axis_index("rep")
    lane_ref[...] = rank + (me % (LANES // depth)) * depth

    rank_hot = (
        lax.broadcasted_iota(jnp.int32, (LANES, n_rows), 0) % depth == rank
    ).astype(jnp.float32).astype(jnp.bfloat16)
    order = total - index_ref[...]
    digit_id = lax.broadcasted_iota(jnp.int32, (EXTRA, n_rows), 0)
    digits = jnp.zeros((EXTRA, n_rows), jnp.float32)
    left, digit = total, 0
    while left > 0:
        value = ((order >> (8 * digit)) & (BASE - 1)).astype(jnp.float32)
        digits = jnp.where(digit_id == digit, value, digits)
        left, digit = left // BASE, digit + 1
    masked = jnp.concatenate(
        [jnp.where(cluster == c, digits, 0.0) for c in range(clusters)], axis=0
    ).astype(jnp.bfloat16)
    coded = nt_dot(masked, rank_hot).astype(jnp.bfloat16)
    send_ref[:, 2 * depth:, :] = coded.reshape(clusters, EXTRA, LANES)

    slot = cluster * depth + rank
    tall = 256
    for t in range(clusters * depth // tall):
        ids = lax.broadcasted_iota(jnp.int32, (tall, n_rows), 0) + t * tall
        place[t * tall:(t + 1) * tall, :] = (ids == slot).astype(jnp.float32).astype(jnp.bfloat16)

    basis_copy.wait()
    for k in range(CHUNKS):
        emb_copy(k).wait()
        part = slice(k * step, (k + 1) * step)
        projected = jnp.dot(emb[part, :], basis[...], preferred_element_type=jnp.float32)
        scale = lax.rsqrt(jnp.sum(projected * projected, axis=1, keepdims=True) + 1e-06)
        rows[part, :] = (projected * scale).astype(jnp.bfloat16)
    packed = jnp.dot(place[...], rows[...], preferred_element_type=jnp.float32).astype(jnp.bfloat16)
    send_ref[:, :depth, :] = packed[:, :LANES].reshape(clusters, depth, LANES)
    send_ref[:, depth:2 * depth, :] = packed[:, LANES:].reshape(clusters, depth, LANES)


def nearest_kernel(recv_ref, out_ref, x, col, *, depth):
    n = recv_ref.shape[0]
    slots = n * depth
    group = LANES // depth
    x[:, :LANES] = recv_ref[:, :depth, :].reshape(slots, LANES)
    x[:, LANES:] = recv_ref[:, depth:2 * depth, :].reshape(slots, LANES)
    digit_id = lax.broadcasted_iota(jnp.int32, (n, EXTRA, LANES), 1)
    weight = jnp.where(
        digit_id == 0, 1.0, jnp.where(digit_id == 1, float(BASE), float(BASE * BASE))
    )
    digits = recv_ref[:, 2 * depth:, :].astype(jnp.float32)
    order = jnp.sum(digits * weight, axis=1)
    lane_group = lax.broadcasted_iota(jnp.int32, (1, LANES), 1) // depth
    rows_of = []
    for k in range(slots // LANES):
        row = order[k * group:k * group + 1, :]
        for q in range(1, group):
            row = jnp.where(lane_group == q, order[k * group + q:k * group + q + 1, :], row)
        rows_of.append(row)
    turned = order.T
    for c in range(n):
        col[c * depth:(c + 1) * depth, :] = jnp.broadcast_to(
            turned[:depth, c:c + 1], (depth, LANES)
        )
    tile = 256
    for i in range(slots // tile):
        right = x[i * tile:(i + 1) * tile, :]
        row = [rows_of[2 * i], rows_of[2 * i + 1]]
        best = [jnp.full((8, LANES), -1.0, jnp.float32) for _ in range(2)]
        for j in range(slots // tile):
            scores = nt_dot(x[j * tile:(j + 1) * tile, :], right)
            here = col[j * tile:(j + 1) * tile, :]
            for h in range(2):
                kept = jnp.where(here > row[h], scores[:, h * LANES:(h + 1) * LANES], -1.0)
                best[h] = jnp.maximum(best[h], jnp.max(kept.reshape(tile // 8, 8, LANES), axis=0))
        for h in range(2):
            top = jnp.max(best[h], axis=0, keepdims=True)
            k = 2 * i + h
            for q in range(group):
                out_ref[k * group + q] = top


def collect_kernel(back_ref, cluster_ref, lane_ref, out_ref):
    n = back_ref.shape[0]
    n_rows = cluster_ref.shape[1]
    back = back_ref[...].reshape(n, LANES)
    high = back.astype(jnp.bfloat16)
    rest = back - high.astype(jnp.float32)
    middle = rest.astype(jnp.bfloat16)
    low = (rest - middle.astype(jnp.float32)).astype(jnp.bfloat16)
    hot = (
        lax.broadcasted_iota(jnp.int32, (LANES, n_rows), 0) == lane_ref[...]
    ).astype(jnp.float32).astype(jnp.bfloat16)
    picked = jnp.dot(high, hot, preferred_element_type=jnp.float32)
    picked = picked + jnp.dot(middle, hot, preferred_element_type=jnp.float32)
    picked = picked + jnp.dot(low, hot, preferred_element_type=jnp.float32)
    mine = lax.broadcasted_iota(jnp.int32, (n, n_rows), 0) == cluster_ref[...]
    out_ref[...] = jnp.sum(jnp.where(mine, picked, 0.0), axis=0, keepdims=True)


def on_device(embeddings, pca_basis, cluster, doc_index):
    n_docs = lax.axis_size("docs")
    n_rep = lax.axis_size("rep")
    n_dev = n_docs * n_rep
    doc_rows, width = embeddings.shape
    features = pca_basis.shape[1]
    clusters = CL_DEV * n_docs
    assert clusters == n_dev and features == 2 * LANES
    depth = max(2, 2 * doc_rows // clusters)
    cluster_row = cluster.reshape(1, doc_rows)
    index_row = doc_index.reshape(1, doc_rows)
    vmem = pl.BlockSpec(memory_space=pltpu.VMEM)
    hbm = pl.BlockSpec(memory_space=pl.ANY)
    message = 2 * depth + EXTRA

    def pack(*refs):
        project_and_pack(*refs, depth=depth, clusters=clusters, total=doc_rows * n_dev)

    send, lane = pl.pallas_call(
        pack,
        name="project_and_pack",
        in_specs=[vmem, vmem, hbm, hbm],
        out_specs=[vmem, vmem],
        out_shape=[
            jax.ShapeDtypeStruct((n_dev, message, LANES), jnp.bfloat16),
            jax.ShapeDtypeStruct((1, doc_rows), jnp.int32),
        ],
        scratch_shapes=[
            pltpu.VMEM((doc_rows, width), jnp.bfloat16),
            pltpu.VMEM((width, features), jnp.bfloat16),
            pltpu.VMEM((doc_rows, features), jnp.bfloat16),
            pltpu.VMEM((clusters * depth, doc_rows), jnp.bfloat16),
            pltpu.SemaphoreType.DMA((CHUNKS,)),
            pltpu.SemaphoreType.DMA,
        ],
    )(cluster_row, index_row, embeddings, pca_basis)
    recv = lax.all_to_all(send, AXES, split_axis=0, concat_axis=0, tiled=True)

    def search(*refs):
        nearest_kernel(*refs, depth=depth)

    found = pl.pallas_call(
        search,
        name="nearest",
        in_specs=[vmem],
        out_specs=vmem,
        out_shape=jax.ShapeDtypeStruct((n_dev, 1, LANES), jnp.float32),
        scratch_shapes=[
            pltpu.VMEM((n_dev * depth, features), jnp.bfloat16),
            pltpu.VMEM((n_dev * depth, LANES), jnp.float32),
        ],
    )(recv)
    back = lax.all_to_all(found, AXES, split_axis=0, concat_axis=0, tiled=True)
    nearest = pl.pallas_call(
        collect_kernel,
        name="collect",
        in_specs=[vmem, vmem, vmem],
        out_specs=vmem,
        out_shape=jax.ShapeDtypeStruct((1, doc_rows), jnp.float32),
    )(back, cluster_row, lane)
    return nearest.reshape(doc_rows)


def solution(mesh):
    return jax.shard_map(
        on_device,
        mesh=mesh,
        in_specs=(P(AXES, None), P(), P(AXES, None), P(AXES)),
        out_specs=P(AXES),
        check_vma=False,
    )
```

```python
import jax
import jax.numpy as jnp
from jax import lax
from jax.experimental import pallas as pl
from jax.experimental.pallas import tpu as pltpu
from jax.sharding import PartitionSpec as P

CL_DEV = 4
AXES = ("docs", "rep")
LANES = 128
EXTRA = 8
CHUNKS = 8
BASE = 256


def nt_dot(a, b):
    return lax.dot_general(a, b, (((1,), (1,)), ((), ())), preferred_element_type=jnp.float32)


def project_and_pack(
    cluster_hbm, index_hbm, emb_hbm, basis_hbm, send_ref, lane_ref,
    cluster_ref, index_ref, emb, basis, rows, place, emb_sem, basis_sem, id_sem, *, depth, clusters, total,
):
    n_rows, width = emb.shape
    features = basis.shape[1]
    step = n_rows // CHUNKS

    def emb_copy(k):
        part = pl.ds(k * step, step)
        return pltpu.make_async_copy(emb_hbm.at[part], emb.at[part], emb_sem.at[k])

    cluster_copy = pltpu.make_async_copy(cluster_hbm, cluster_ref, id_sem.at[0])
    index_copy = pltpu.make_async_copy(index_hbm, index_ref, id_sem.at[1])
    cluster_copy.start()
    index_copy.start()
    basis_copy = pltpu.make_async_copy(basis_hbm, basis, basis_sem)
    basis_copy.start()
    for k in range(CHUNKS):
        emb_copy(k).start()

    cluster_copy.wait()
    index_copy.wait()
    cluster = cluster_ref[...]
    blocks = n_rows // LANES
    cluster_iota = lax.broadcasted_iota(jnp.int32, (clusters, n_rows), 0)
    member = cluster_iota == cluster
    member_f = member.astype(jnp.float32)
    stacked = jnp.concatenate(
        [member_f[:, b * LANES:(b + 1) * LANES] for b in range(blocks)], axis=0
    ).astype(jnp.bfloat16)
    row_id = lax.broadcasted_iota(jnp.int32, (LANES, 2 * LANES), 0)
    col_id = lax.broadcasted_iota(jnp.int32, (LANES, 2 * LANES), 1)
    earlier = ((row_id < col_id) | (col_id >= LANES)).astype(jnp.float32).astype(jnp.bfloat16)
    prefix = jnp.dot(stacked, earlier, preferred_element_type=jnp.float32)
    carry = jnp.zeros((clusters, LANES), jnp.float32)
    ranks = []
    for b in range(blocks):
        part = prefix[b * clusters:(b + 1) * clusters]
        mine = member_f[:, b * LANES:(b + 1) * LANES]
        ranks.append(jnp.sum(mine * (part[:, :LANES] + carry), axis=0, keepdims=True))
        carry = carry + part[:, LANES:]
    rank = jnp.concatenate(ranks, axis=1).astype(jnp.int32)
    me = lax.axis_index("docs") * lax.axis_size("rep") + lax.axis_index("rep")
    lane_ref[...] = rank + (me % (LANES // depth)) * depth

    rank_hot = (
        lax.broadcasted_iota(jnp.int32, (LANES, n_rows), 0) % depth == rank
    ).astype(jnp.float32).astype(jnp.bfloat16)
    order = total - index_ref[...]
    digit_id = lax.broadcasted_iota(jnp.int32, (EXTRA, n_rows), 0)
    digits = jnp.zeros((EXTRA, n_rows), jnp.float32)
    left, digit = total, 0
    while left > 0:
        value = ((order >> (8 * digit)) & (BASE - 1)).astype(jnp.float32)
        digits = jnp.where(digit_id == digit, value, digits)
        left, digit = left // BASE, digit + 1
    masked = jnp.concatenate(
        [jnp.where(cluster == c, digits, 0.0) for c in range(clusters)], axis=0
    ).astype(jnp.bfloat16)
    coded = nt_dot(masked, rank_hot).astype(jnp.bfloat16)
    send_ref[:, 2 * depth:, :] = coded.reshape(clusters, EXTRA, LANES)

    seat = lax.broadcasted_iota(jnp.int32, (depth, n_rows), 0).astype(jnp.float32).astype(jnp.bfloat16)
    one = jnp.ones((depth, n_rows), jnp.bfloat16)
    none = jnp.zeros((depth, n_rows), jnp.bfloat16)
    for c in range(clusters):
        here = jnp.where(cluster == c, rank.astype(jnp.float32), -1.0).astype(jnp.bfloat16)
        place[c * depth:(c + 1) * depth, :] = jnp.where(seat == here, one, none)

    basis_copy.wait()
    for k in range(CHUNKS):
        emb_copy(k).wait()
    halves = 2
    step = n_rows // halves
    for k in range(halves):
        part = slice(k * step, (k + 1) * step)
        projected = jnp.dot(emb[part, :], basis[...], preferred_element_type=jnp.float32)
        scale = lax.rsqrt(jnp.sum(projected * projected, axis=1, keepdims=True) + 1e-06)
        rows[part, :] = (projected * scale).astype(jnp.bfloat16)
    packed = jnp.dot(place[...], rows[...], preferred_element_type=jnp.float32).astype(jnp.bfloat16)
    send_ref[:, :depth, :] = packed[:, :LANES].reshape(clusters, depth, LANES)
    send_ref[:, depth:2 * depth, :] = packed[:, LANES:].reshape(clusters, depth, LANES)


def nearest_kernel(recv_ref, out_ref, x, col, *, depth):
    n = recv_ref.shape[0]
    slots = n * depth
    group = LANES // depth
    x[:, :LANES] = recv_ref[:, :depth, :].reshape(slots, LANES)
    x[:, LANES:] = recv_ref[:, depth:2 * depth, :].reshape(slots, LANES)
    digit_id = lax.broadcasted_iota(jnp.int32, (n, EXTRA, LANES), 1)
    weight = jnp.where(
        digit_id == 0, 1.0, jnp.where(digit_id == 1, float(BASE), float(BASE * BASE))
    )
    digits = recv_ref[:, 2 * depth:, :].astype(jnp.float32)
    order = jnp.sum(digits * weight, axis=1)
    lane_group = lax.broadcasted_iota(jnp.int32, (1, LANES), 1) // depth
    rows_of = []
    for k in range(slots // LANES):
        row = order[k * group:k * group + 1, :]
        for q in range(1, group):
            row = jnp.where(lane_group == q, order[k * group + q:k * group + q + 1, :], row)
        rows_of.append(row)
    turned = order.T
    for c in range(n):
        col[c * depth:(c + 1) * depth, :] = jnp.broadcast_to(
            turned[:depth, c:c + 1], (depth, LANES)
        )
    tile = 256
    for i in range(slots // tile):
        right = x[i * tile:(i + 1) * tile, :]
        row = [rows_of[2 * i], rows_of[2 * i + 1]]
        best = [jnp.full((8, LANES), -1.0, jnp.float32) for _ in range(2)]
        for j in range(slots // tile):
            scores = nt_dot(x[j * tile:(j + 1) * tile, :], right)
            here = col[j * tile:(j + 1) * tile, :]
            for h in range(2):
                kept = jnp.where(here > row[h], scores[:, h * LANES:(h + 1) * LANES], -1.0)
                best[h] = jnp.maximum(best[h], jnp.max(kept.reshape(tile // 8, 8, LANES), axis=0))
        for h in range(2):
            top = jnp.max(best[h], axis=0, keepdims=True)
            k = 2 * i + h
            for q in range(group):
                out_ref[k * group + q] = top


def collect_kernel(back_ref, cluster_ref, lane_ref, out_ref):
    n = back_ref.shape[0]
    n_rows = cluster_ref.shape[1]
    back = back_ref[...].reshape(n, LANES)
    high = back.astype(jnp.bfloat16)
    rest = back - high.astype(jnp.float32)
    middle = rest.astype(jnp.bfloat16)
    low = (rest - middle.astype(jnp.float32)).astype(jnp.bfloat16)
    hot = (
        lax.broadcasted_iota(jnp.int32, (LANES, n_rows), 0) == lane_ref[...]
    ).astype(jnp.float32).astype(jnp.bfloat16)
    picked = jnp.dot(high, hot, preferred_element_type=jnp.float32)
    picked = picked + jnp.dot(middle, hot, preferred_element_type=jnp.float32)
    picked = picked + jnp.dot(low, hot, preferred_element_type=jnp.float32)
    mine = lax.broadcasted_iota(jnp.int32, (n, n_rows), 0) == cluster_ref[...]
    out_ref[...] = jnp.sum(jnp.where(mine, picked, 0.0), axis=0, keepdims=True)


def on_device(embeddings, pca_basis, cluster, doc_index):
    n_docs = lax.axis_size("docs")
    n_rep = lax.axis_size("rep")
    n_dev = n_docs * n_rep
    doc_rows, width = embeddings.shape
    features = pca_basis.shape[1]
    clusters = CL_DEV * n_docs
    assert clusters == n_dev and features == 2 * LANES
    depth = max(2, 2 * doc_rows // clusters)
    cluster_row = cluster.reshape(1, doc_rows)
    index_row = doc_index.reshape(1, doc_rows)
    vmem = pl.BlockSpec(memory_space=pltpu.VMEM)
    hbm = pl.BlockSpec(memory_space=pltpu.HBM)
    message = 2 * depth + EXTRA

    def pack(*refs):
        project_and_pack(*refs, depth=depth, clusters=clusters, total=doc_rows * n_dev)

    send, lane = pl.pallas_call(
        pack,
        name="project_and_pack",
        compiler_params=pltpu.CompilerParams(vmem_limit_bytes=28 * 2**20),
        in_specs=[hbm, hbm, hbm, hbm],
        out_specs=[vmem, vmem],
        out_shape=[
            jax.ShapeDtypeStruct((n_dev, message, LANES), jnp.bfloat16),
            jax.ShapeDtypeStruct((1, doc_rows), jnp.int32),
        ],
        scratch_shapes=[
            pltpu.VMEM((1, doc_rows), jnp.int32),
            pltpu.VMEM((1, doc_rows), jnp.int32),
            pltpu.VMEM((doc_rows, width), jnp.bfloat16),
            pltpu.VMEM((width, features), jnp.bfloat16),
            pltpu.VMEM((doc_rows, features), jnp.bfloat16),
            pltpu.VMEM((clusters * depth, doc_rows), jnp.bfloat16),
            pltpu.SemaphoreType.DMA((CHUNKS,)),
            pltpu.SemaphoreType.DMA,
            pltpu.SemaphoreType.DMA((2,)),
        ],
    )(*[pltpu.with_memory_space_constraint(a, pltpu.HBM) for a in (cluster_row, index_row, embeddings, pca_basis)])
    recv = lax.all_to_all(send, AXES, split_axis=0, concat_axis=0, tiled=True)

    def search(*refs):
        nearest_kernel(*refs, depth=depth)

    found = pl.pallas_call(
        search,
        name="nearest",
        compiler_params=pltpu.CompilerParams(vmem_limit_bytes=16 * 2**20),
        in_specs=[vmem],
        out_specs=vmem,
        out_shape=jax.ShapeDtypeStruct((n_dev, 1, LANES), jnp.float32),
        scratch_shapes=[
            pltpu.VMEM((n_dev * depth, features), jnp.bfloat16),
            pltpu.VMEM((n_dev * depth, LANES), jnp.float32),
        ],
    )(recv)
    back = lax.all_to_all(found, AXES, split_axis=0, concat_axis=0, tiled=True)
    nearest = pl.pallas_call(
        collect_kernel,
        name="collect",
        compiler_params=pltpu.CompilerParams(vmem_limit_bytes=8 * 2**20),
        in_specs=[vmem, vmem, vmem],
        out_specs=vmem,
        out_shape=jax.ShapeDtypeStruct((1, doc_rows), jnp.float32),
    )(back, cluster_row, lane)
    return nearest.reshape(doc_rows)


def solution(mesh):
    return jax.shard_map(
        on_device,
        mesh=mesh,
        in_specs=(P(AXES, None), P(), P(AXES, None), P(AXES)),
        out_specs=P(AXES),
        check_vma=False,
    )
```

```python
import jax
import jax.numpy as jnp
from jax import lax
from jax.experimental import pallas as pl
from jax.experimental.pallas import tpu as pltpu
from jax.sharding import PartitionSpec as P

CL_DEV = 4
AXES = ("docs", "rep")
LANES = 128
EXTRA = 8
CHUNKS = 8
FIRST = 4
BASE = 256


def nt_dot(a, b):
    return lax.dot_general(a, b, (((1,), (1,)), ((), ())), preferred_element_type=jnp.float32)


def project_and_pack(
    cluster_hbm, index_hbm, emb_hbm, basis_hbm, send_ref, lane_ref,
    cluster_ref, index_ref, emb, basis, rows, place, emb_sem, basis_sem, id_sem, *, depth, clusters, total,
):
    n_rows, width = emb.shape
    features = basis.shape[1]
    step = n_rows // CHUNKS

    def emb_copy(k):
        part = pl.ds(k * step, step)
        return pltpu.make_async_copy(emb_hbm.at[part], emb.at[part], emb_sem.at[k])

    cluster_copy = pltpu.make_async_copy(cluster_hbm, cluster_ref, id_sem.at[0])
    index_copy = pltpu.make_async_copy(index_hbm, index_ref, id_sem.at[1])
    cluster_copy.start()
    index_copy.start()
    basis_copy = pltpu.make_async_copy(basis_hbm, basis, basis_sem)
    basis_copy.start()
    for k in range(CHUNKS):
        emb_copy(k).start(priority=0 if k < FIRST else 1)

    cluster_copy.wait()
    index_copy.wait()
    cluster = cluster_ref[...]
    blocks = n_rows // LANES
    cluster_iota = lax.broadcasted_iota(jnp.int32, (clusters, n_rows), 0)
    member = cluster_iota == cluster
    member_f = member.astype(jnp.float32)
    stacked = jnp.concatenate(
        [member_f[:, b * LANES:(b + 1) * LANES] for b in range(blocks)], axis=0
    ).astype(jnp.bfloat16)
    row_id = lax.broadcasted_iota(jnp.int32, (LANES, 2 * LANES), 0)
    col_id = lax.broadcasted_iota(jnp.int32, (LANES, 2 * LANES), 1)
    earlier = ((row_id < col_id) | (col_id >= LANES)).astype(jnp.float32).astype(jnp.bfloat16)
    prefix = jnp.dot(stacked, earlier, preferred_element_type=jnp.float32)
    carry = jnp.zeros((clusters, LANES), jnp.float32)
    ranks = []
    for b in range(blocks):
        part = prefix[b * clusters:(b + 1) * clusters]
        mine = member_f[:, b * LANES:(b + 1) * LANES]
        ranks.append(jnp.sum(mine * (part[:, :LANES] + carry), axis=0, keepdims=True))
        carry = carry + part[:, LANES:]
    rank = jnp.concatenate(ranks, axis=1).astype(jnp.int32)
    me = lax.axis_index("docs") * lax.axis_size("rep") + lax.axis_index("rep")
    lane_ref[...] = rank + (me % (LANES // depth)) * depth

    rank_hot = (
        lax.broadcasted_iota(jnp.int32, (LANES, n_rows), 0) % depth == rank
    ).astype(jnp.float32).astype(jnp.bfloat16)
    order = total - index_ref[...]
    digit_id = lax.broadcasted_iota(jnp.int32, (EXTRA, n_rows), 0)
    digits = jnp.zeros((EXTRA, n_rows), jnp.float32)
    left, digit = total, 0
    while left > 0:
        value = ((order >> (8 * digit)) & (BASE - 1)).astype(jnp.float32)
        digits = jnp.where(digit_id == digit, value, digits)
        left, digit = left // BASE, digit + 1
    masked = jnp.concatenate(
        [jnp.where(cluster == c, digits, 0.0) for c in range(clusters)], axis=0
    ).astype(jnp.bfloat16)
    coded = nt_dot(masked, rank_hot).astype(jnp.bfloat16)
    send_ref[:, 2 * depth:, :] = coded.reshape(clusters, EXTRA, LANES)

    seat = lax.broadcasted_iota(jnp.int32, (depth, n_rows), 0).astype(jnp.float32).astype(jnp.bfloat16)
    one = jnp.ones((depth, n_rows), jnp.bfloat16)
    none = jnp.zeros((depth, n_rows), jnp.bfloat16)
    for c in range(clusters):
        here = jnp.where(cluster == c, rank.astype(jnp.float32), -1.0).astype(jnp.bfloat16)
        place[c * depth:(c + 1) * depth, :] = jnp.where(seat == here, one, none)

    basis_copy.wait()
    size = 256
    for k in range(n_rows // size):
        if k * size == 0:
            for q in range(FIRST):
                emb_copy(q).wait()
        if k * size == FIRST * step:
            for q in range(FIRST, CHUNKS):
                emb_copy(q).wait()
        part = slice(k * size, (k + 1) * size)
        projected = jnp.dot(emb[part, :], basis[...], preferred_element_type=jnp.float32)
        scale = lax.rsqrt(jnp.sum(projected * projected, axis=1, keepdims=True) + 1e-06)
        rows[part, :] = (projected * scale).astype(jnp.bfloat16)
    packed = jnp.dot(place[...], rows[...], preferred_element_type=jnp.float32).astype(jnp.bfloat16)
    send_ref[:, :depth, :] = packed[:, :LANES].reshape(clusters, depth, LANES)
    send_ref[:, depth:2 * depth, :] = packed[:, LANES:].reshape(clusters, depth, LANES)


def nearest_kernel(recv_ref, out_ref, x, col, *, depth):
    n = recv_ref.shape[0]
    slots = n * depth
    group = LANES // depth
    x[:, :LANES] = recv_ref[:, :depth, :].reshape(slots, LANES)
    x[:, LANES:] = recv_ref[:, depth:2 * depth, :].reshape(slots, LANES)
    digit_id = lax.broadcasted_iota(jnp.int32, (n, EXTRA, LANES), 1)
    weight = jnp.where(
        digit_id == 0, 1.0, jnp.where(digit_id == 1, float(BASE), float(BASE * BASE))
    )
    digits = recv_ref[:, 2 * depth:, :].astype(jnp.float32)
    order = jnp.sum(digits * weight, axis=1)
    lane_group = lax.broadcasted_iota(jnp.int32, (1, LANES), 1) // depth
    rows_of = []
    for k in range(slots // LANES):
        row = order[k * group:k * group + 1, :]
        for q in range(1, group):
            row = jnp.where(lane_group == q, order[k * group + q:k * group + q + 1, :], row)
        rows_of.append(row)
    turned = order.T
    for c in range(n):
        col[c * depth:(c + 1) * depth, :] = jnp.broadcast_to(
            turned[:depth, c:c + 1], (depth, LANES)
        )
    tile = 256
    for i in range(slots // tile):
        right = x[i * tile:(i + 1) * tile, :]
        row = [rows_of[2 * i], rows_of[2 * i + 1]]
        best = [jnp.full((8, LANES), -1.0, jnp.float32) for _ in range(2)]
        for j in range(slots // tile):
            scores = nt_dot(x[j * tile:(j + 1) * tile, :], right)
            here = col[j * tile:(j + 1) * tile, :]
            for h in range(2):
                kept = jnp.where(here > row[h], scores[:, h * LANES:(h + 1) * LANES], -1.0)
                best[h] = jnp.maximum(best[h], jnp.max(kept.reshape(tile // 8, 8, LANES), axis=0))
        for h in range(2):
            top = jnp.max(best[h], axis=0, keepdims=True)
            k = 2 * i + h
            for q in range(group):
                out_ref[k * group + q] = top


def collect_kernel(back_ref, cluster_ref, lane_ref, out_ref):
    n = back_ref.shape[0]
    n_rows = cluster_ref.shape[1]
    back = back_ref[...].reshape(n, LANES)
    high = back.astype(jnp.bfloat16)
    rest = back - high.astype(jnp.float32)
    middle = rest.astype(jnp.bfloat16)
    low = (rest - middle.astype(jnp.float32)).astype(jnp.bfloat16)
    hot = (
        lax.broadcasted_iota(jnp.int32, (LANES, n_rows), 0) == lane_ref[...]
    ).astype(jnp.float32).astype(jnp.bfloat16)
    picked = jnp.dot(high, hot, preferred_element_type=jnp.float32)
    picked = picked + jnp.dot(middle, hot, preferred_element_type=jnp.float32)
    picked = picked + jnp.dot(low, hot, preferred_element_type=jnp.float32)
    mine = lax.broadcasted_iota(jnp.int32, (n, n_rows), 0) == cluster_ref[...]
    out_ref[...] = jnp.sum(jnp.where(mine, picked, 0.0), axis=0, keepdims=True)


def on_device(embeddings, pca_basis, cluster, doc_index):
    n_docs = lax.axis_size("docs")
    n_rep = lax.axis_size("rep")
    n_dev = n_docs * n_rep
    doc_rows, width = embeddings.shape
    features = pca_basis.shape[1]
    clusters = CL_DEV * n_docs
    assert clusters == n_dev and features == 2 * LANES
    depth = max(2, 2 * doc_rows // clusters)
    cluster_row = cluster.reshape(1, doc_rows)
    index_row = doc_index.reshape(1, doc_rows)
    vmem = pl.BlockSpec(memory_space=pltpu.VMEM)
    hbm = pl.BlockSpec(memory_space=pltpu.HBM)
    message = 2 * depth + EXTRA

    def pack(*refs):
        project_and_pack(*refs, depth=depth, clusters=clusters, total=doc_rows * n_dev)

    send, lane = pl.pallas_call(
        pack,
        name="project_and_pack",
        compiler_params=pltpu.CompilerParams(vmem_limit_bytes=28 * 2**20),
        in_specs=[hbm, hbm, hbm, hbm],
        out_specs=[vmem, vmem],
        out_shape=[
            jax.ShapeDtypeStruct((n_dev, message, LANES), jnp.bfloat16),
            jax.ShapeDtypeStruct((1, doc_rows), jnp.int32),
        ],
        scratch_shapes=[
            pltpu.VMEM((1, doc_rows), jnp.int32),
            pltpu.VMEM((1, doc_rows), jnp.int32),
            pltpu.VMEM((doc_rows, width), jnp.bfloat16),
            pltpu.VMEM((width, features), jnp.bfloat16),
            pltpu.VMEM((doc_rows, features), jnp.bfloat16),
            pltpu.VMEM((clusters * depth, doc_rows), jnp.bfloat16),
            pltpu.SemaphoreType.DMA((CHUNKS,)),
            pltpu.SemaphoreType.DMA,
            pltpu.SemaphoreType.DMA((2,)),
        ],
    )(*[pltpu.with_memory_space_constraint(a, pltpu.HBM) for a in (cluster_row, index_row, embeddings, pca_basis)])
    recv = lax.all_to_all(send, AXES, split_axis=0, concat_axis=0, tiled=True)

    def search(*refs):
        nearest_kernel(*refs, depth=depth)

    found = pl.pallas_call(
        search,
        name="nearest",
        compiler_params=pltpu.CompilerParams(vmem_limit_bytes=16 * 2**20),
        in_specs=[vmem],
        out_specs=vmem,
        out_shape=jax.ShapeDtypeStruct((n_dev, 1, LANES), jnp.float32),
        scratch_shapes=[
            pltpu.VMEM((n_dev * depth, features), jnp.bfloat16),
            pltpu.VMEM((n_dev * depth, LANES), jnp.float32),
        ],
    )(recv)
    back = lax.all_to_all(found, AXES, split_axis=0, concat_axis=0, tiled=True)
    nearest = pl.pallas_call(
        collect_kernel,
        name="collect",
        compiler_params=pltpu.CompilerParams(vmem_limit_bytes=8 * 2**20),
        in_specs=[vmem, vmem, vmem],
        out_specs=vmem,
        out_shape=jax.ShapeDtypeStruct((1, doc_rows), jnp.float32),
    )(back, cluster_row, lane)
    return nearest.reshape(doc_rows)


def solution(mesh):
    return jax.shard_map(
        on_device,
        mesh=mesh,
        in_specs=(P(AXES, None), P(), P(AXES, None), P(AXES)),
        out_specs=P(AXES),
        check_vma=False,
    )
```

```python
import jax
import jax.numpy as jnp
from jax import lax
from jax.experimental import pallas as pl
from jax.experimental.pallas import tpu as pltpu
from jax.sharding import PartitionSpec as P

CL_DEV = 4
AXES = ("docs", "rep")
LANES = 128
PAIR = 2
CHUNKS = 8
FIRST = 4
BASE = 256


def extra_rows(total):
    digits = 1
    while BASE ** digits <= total:
        digits += 1
    return -(-digits // PAIR) * PAIR


def nt_dot(a, b):
    return lax.dot_general(a, b, (((1,), (1,)), ((), ())), preferred_element_type=jnp.float32)


def project_and_pack(
    cluster_hbm, index_hbm, emb_hbm, basis_hbm, send_pairs, lane_ref,
    cluster_ref, index_ref, emb, basis, rows, place, emb_sem, basis_sem, id_sem, *, depth, clusters, total,
):
    extra = extra_rows(total)
    send_ref = send_pairs.reshape(clusters, 2 * depth + extra, LANES)
    n_rows, width = emb.shape
    features = basis.shape[1]
    step = n_rows // CHUNKS

    def emb_copy(k):
        part = pl.ds(k * step, step)
        return pltpu.make_async_copy(emb_hbm.at[part], emb.at[part], emb_sem.at[k])

    cluster_copy = pltpu.make_async_copy(cluster_hbm, cluster_ref, id_sem.at[0])
    index_copy = pltpu.make_async_copy(index_hbm, index_ref, id_sem.at[1])
    cluster_copy.start()
    index_copy.start()
    basis_copy = pltpu.make_async_copy(basis_hbm, basis, basis_sem)
    basis_copy.start()
    for k in range(CHUNKS):
        emb_copy(k).start(priority=0 if k < FIRST else 1)

    cluster_copy.wait()
    index_copy.wait()
    cluster = cluster_ref[...]
    blocks = n_rows // LANES
    cluster_iota = lax.broadcasted_iota(jnp.int32, (clusters, n_rows), 0)
    member = cluster_iota == cluster
    member_f = member.astype(jnp.float32)
    stacked = jnp.concatenate(
        [member_f[:, b * LANES:(b + 1) * LANES] for b in range(blocks)], axis=0
    ).astype(jnp.bfloat16)
    row_id = lax.broadcasted_iota(jnp.int32, (LANES, 2 * LANES), 0)
    col_id = lax.broadcasted_iota(jnp.int32, (LANES, 2 * LANES), 1)
    earlier = ((row_id < col_id) | (col_id >= LANES)).astype(jnp.float32).astype(jnp.bfloat16)
    prefix = jnp.dot(stacked, earlier, preferred_element_type=jnp.float32)
    carry = jnp.zeros((clusters, LANES), jnp.float32)
    ranks = []
    for b in range(blocks):
        part = prefix[b * clusters:(b + 1) * clusters]
        mine = member_f[:, b * LANES:(b + 1) * LANES]
        ranks.append(jnp.sum(mine * (part[:, :LANES] + carry), axis=0, keepdims=True))
        carry = carry + part[:, LANES:]
    rank = jnp.concatenate(ranks, axis=1).astype(jnp.int32)
    me = lax.axis_index("docs") * lax.axis_size("rep") + lax.axis_index("rep")
    lane_ref[...] = rank + (me % (LANES // depth)) * depth

    rank_hot = (
        lax.broadcasted_iota(jnp.int32, (LANES, n_rows), 0) % depth == rank
    ).astype(jnp.float32).astype(jnp.bfloat16)
    order = total - index_ref[...]
    digit_id = lax.broadcasted_iota(jnp.int32, (extra, n_rows), 0)
    digits = jnp.zeros((extra, n_rows), jnp.float32)
    left, digit = total, 0
    while left > 0:
        value = ((order >> (8 * digit)) & (BASE - 1)).astype(jnp.float32)
        digits = jnp.where(digit_id == digit, value, digits)
        left, digit = left // BASE, digit + 1
    masked = jnp.concatenate(
        [jnp.where(cluster == c, digits, 0.0) for c in range(clusters)], axis=0
    ).astype(jnp.bfloat16)
    coded = nt_dot(masked, rank_hot).astype(jnp.bfloat16)
    for c in range(clusters):
        send_ref[c, 2 * depth:, :] = coded[c * extra:(c + 1) * extra, :]

    seat = lax.broadcasted_iota(jnp.int32, (depth, n_rows), 0).astype(jnp.float32).astype(jnp.bfloat16)
    one = jnp.ones((depth, n_rows), jnp.bfloat16)
    none = jnp.zeros((depth, n_rows), jnp.bfloat16)
    for c in range(clusters):
        here = jnp.where(cluster == c, rank.astype(jnp.float32), -1.0).astype(jnp.bfloat16)
        place[c * depth:(c + 1) * depth, :] = jnp.where(seat == here, one, none)

    basis_copy.wait()
    size = 256
    for k in range(n_rows // size):
        if k * size == 0:
            for q in range(FIRST):
                emb_copy(q).wait()
        if k * size == FIRST * step:
            for q in range(FIRST, CHUNKS):
                emb_copy(q).wait()
        part = slice(k * size, (k + 1) * size)
        projected = jnp.dot(emb[part, :], basis[...], preferred_element_type=jnp.float32)
        scale = lax.rsqrt(jnp.sum(projected * projected, axis=1, keepdims=True) + 1e-06)
        rows[part, :] = (projected * scale).astype(jnp.bfloat16)
    packed = jnp.dot(place[...], rows[...], preferred_element_type=jnp.float32).astype(jnp.bfloat16)
    send_ref[:, :depth, :] = packed[:, :LANES].reshape(clusters, depth, LANES)
    send_ref[:, depth:2 * depth, :] = packed[:, LANES:].reshape(clusters, depth, LANES)


def nearest_kernel(recv_pairs, out_ref, x, col, *, depth):
    n, pairs = recv_pairs.shape[:2]
    recv_ref = recv_pairs.reshape(n, pairs * PAIR, LANES)
    extra = pairs * PAIR - 2 * depth
    slots = n * depth
    group = LANES // depth
    x[:, :LANES] = recv_ref[:, :depth, :].reshape(slots, LANES)
    x[:, LANES:] = recv_ref[:, depth:2 * depth, :].reshape(slots, LANES)
    digit_id = lax.broadcasted_iota(jnp.int32, (n, extra, LANES), 1)
    weight = jnp.where(
        digit_id == 0, 1.0, jnp.where(digit_id == 1, float(BASE), float(BASE * BASE))
    )
    digits = recv_ref[:, 2 * depth:, :].astype(jnp.float32)
    order = jnp.sum(digits * weight, axis=1)
    lane_group = lax.broadcasted_iota(jnp.int32, (1, LANES), 1) // depth
    rows_of = []
    for k in range(slots // LANES):
        row = order[k * group:k * group + 1, :]
        for q in range(1, group):
            row = jnp.where(lane_group == q, order[k * group + q:k * group + q + 1, :], row)
        rows_of.append(row)
    turned = order.T
    for c in range(n):
        col[c * depth:(c + 1) * depth, :] = jnp.broadcast_to(
            turned[:depth, c:c + 1], (depth, LANES)
        )
    tile = 256
    for i in range(slots // tile):
        right = x[i * tile:(i + 1) * tile, :]
        row = [rows_of[2 * i], rows_of[2 * i + 1]]
        best = [jnp.full((8, LANES), -1.0, jnp.float32) for _ in range(2)]
        for j in range(slots // tile):
            scores = nt_dot(x[j * tile:(j + 1) * tile, :], right)
            here = col[j * tile:(j + 1) * tile, :]
            for h in range(2):
                kept = jnp.where(here > row[h], scores[:, h * LANES:(h + 1) * LANES], -1.0)
                best[h] = jnp.maximum(best[h], jnp.max(kept.reshape(tile // 8, 8, LANES), axis=0))
        for h in range(2):
            top = jnp.max(best[h], axis=0, keepdims=True)
            k = 2 * i + h
            for q in range(group):
                out_ref[k * group + q] = top


def collect_kernel(back_ref, cluster_ref, lane_ref, out_ref):
    n = back_ref.shape[0]
    n_rows = cluster_ref.shape[1]
    back = back_ref[...].reshape(n, LANES)
    high = back.astype(jnp.bfloat16)
    rest = back - high.astype(jnp.float32)
    middle = rest.astype(jnp.bfloat16)
    low = (rest - middle.astype(jnp.float32)).astype(jnp.bfloat16)
    hot = (
        lax.broadcasted_iota(jnp.int32, (LANES, n_rows), 0) == lane_ref[...]
    ).astype(jnp.float32).astype(jnp.bfloat16)
    picked = jnp.dot(high, hot, preferred_element_type=jnp.float32)
    picked = picked + jnp.dot(middle, hot, preferred_element_type=jnp.float32)
    picked = picked + jnp.dot(low, hot, preferred_element_type=jnp.float32)
    mine = lax.broadcasted_iota(jnp.int32, (n, n_rows), 0) == cluster_ref[...]
    out_ref[...] = jnp.sum(jnp.where(mine, picked, 0.0), axis=0, keepdims=True)


def on_device(embeddings, pca_basis, cluster, doc_index):
    n_docs = lax.axis_size("docs")
    n_rep = lax.axis_size("rep")
    n_dev = n_docs * n_rep
    doc_rows, width = embeddings.shape
    features = pca_basis.shape[1]
    clusters = CL_DEV * n_docs
    assert clusters == n_dev and features == 2 * LANES
    depth = max(2, 2 * doc_rows // clusters)
    cluster_row = cluster.reshape(1, doc_rows)
    index_row = doc_index.reshape(1, doc_rows)
    vmem = pl.BlockSpec(memory_space=pltpu.VMEM)
    hbm = pl.BlockSpec(memory_space=pltpu.HBM)
    message = 2 * depth + extra_rows(doc_rows * n_dev)

    def pack(*refs):
        project_and_pack(*refs, depth=depth, clusters=clusters, total=doc_rows * n_dev)

    send, lane = pl.pallas_call(
        pack,
        name="project_and_pack",
        compiler_params=pltpu.CompilerParams(vmem_limit_bytes=28 * 2**20),
        in_specs=[hbm, hbm, hbm, hbm],
        out_specs=[vmem, vmem],
        out_shape=[
            jax.ShapeDtypeStruct((n_dev, message // PAIR, PAIR, LANES), jnp.bfloat16),
            jax.ShapeDtypeStruct((1, doc_rows), jnp.int32),
        ],
        scratch_shapes=[
            pltpu.VMEM((1, doc_rows), jnp.int32),
            pltpu.VMEM((1, doc_rows), jnp.int32),
            pltpu.VMEM((doc_rows, width), jnp.bfloat16),
            pltpu.VMEM((width, features), jnp.bfloat16),
            pltpu.VMEM((doc_rows, features), jnp.bfloat16),
            pltpu.VMEM((clusters * depth, doc_rows), jnp.bfloat16),
            pltpu.SemaphoreType.DMA((CHUNKS,)),
            pltpu.SemaphoreType.DMA,
            pltpu.SemaphoreType.DMA((2,)),
        ],
    )(*[pltpu.with_memory_space_constraint(a, pltpu.HBM) for a in (cluster_row, index_row, embeddings, pca_basis)])
    recv = lax.all_to_all(send, AXES, split_axis=0, concat_axis=0, tiled=True)

    def search(*refs):
        nearest_kernel(*refs, depth=depth)

    found = pl.pallas_call(
        search,
        name="nearest",
        compiler_params=pltpu.CompilerParams(vmem_limit_bytes=16 * 2**20),
        in_specs=[vmem],
        out_specs=vmem,
        out_shape=jax.ShapeDtypeStruct((n_dev, 1, LANES), jnp.float32),
        scratch_shapes=[
            pltpu.VMEM((n_dev * depth, features), jnp.bfloat16),
            pltpu.VMEM((n_dev * depth, LANES), jnp.float32),
        ],
    )(recv)
    back = lax.all_to_all(found, AXES, split_axis=0, concat_axis=0, tiled=True)
    nearest = pl.pallas_call(
        collect_kernel,
        name="collect",
        compiler_params=pltpu.CompilerParams(vmem_limit_bytes=8 * 2**20),
        in_specs=[vmem, vmem, vmem],
        out_specs=vmem,
        out_shape=jax.ShapeDtypeStruct((1, doc_rows), jnp.float32),
    )(back, cluster_row, lane)
    return nearest.reshape(doc_rows)


def solution(mesh):
    return jax.shard_map(
        on_device,
        mesh=mesh,
        in_specs=(P(AXES, None), P(), P(AXES, None), P(AXES)),
        out_specs=P(AXES),
        check_vma=False,
    )
```

```python
import jax
import jax.numpy as jnp
from jax import lax
from jax.experimental import pallas as pl
from jax.experimental.pallas import tpu as pltpu
from jax.sharding import PartitionSpec as P

CL_DEV = 4
AXES = ("docs", "rep")
LANES = 128
ROWS = 4
CHUNKS = 8
FIRST = 4
BASE = 256


def extra_rows(total):
    digits = 1
    while BASE ** digits <= total:
        digits += 1
    return -(-digits // ROWS) * ROWS


def nt_dot(a, b):
    return lax.dot_general(a, b, (((1,), (1,)), ((), ())), preferred_element_type=jnp.float32)


def project_and_pack(
    cluster_hbm, index_hbm, emb_hbm, basis_hbm, send_rows, lane_ref,
    cluster_ref, index_ref, emb, basis, rows, place, emb_sem, basis_sem, id_sem, *, depth, clusters, total,
):
    extra = extra_rows(total)
    send_ref = send_rows.reshape(clusters, 2 * depth + extra, LANES)
    n_rows, width = emb.shape
    features = basis.shape[1]
    step = n_rows // CHUNKS

    def emb_copy(k):
        part = pl.ds(k * step, step)
        return pltpu.make_async_copy(emb_hbm.at[part], emb.at[part], emb_sem.at[k])

    cluster_copy = pltpu.make_async_copy(cluster_hbm, cluster_ref, id_sem.at[0])
    index_copy = pltpu.make_async_copy(index_hbm, index_ref, id_sem.at[1])
    cluster_copy.start()
    index_copy.start()
    basis_copy = pltpu.make_async_copy(basis_hbm, basis, basis_sem)
    basis_copy.start()
    for k in range(CHUNKS):
        emb_copy(k).start(priority=0 if k < FIRST else 1)

    cluster_copy.wait()
    index_copy.wait()
    cluster = cluster_ref[...]
    blocks = n_rows // LANES
    cluster_iota = lax.broadcasted_iota(jnp.int32, (clusters, n_rows), 0)
    member = cluster_iota == cluster
    member_f = member.astype(jnp.float32)
    stacked = jnp.concatenate(
        [member_f[:, b * LANES:(b + 1) * LANES] for b in range(blocks)], axis=0
    ).astype(jnp.bfloat16)
    row_id = lax.broadcasted_iota(jnp.int32, (LANES, 2 * LANES), 0)
    col_id = lax.broadcasted_iota(jnp.int32, (LANES, 2 * LANES), 1)
    earlier = ((row_id < col_id) | (col_id >= LANES)).astype(jnp.float32).astype(jnp.bfloat16)
    prefix = jnp.dot(stacked, earlier, preferred_element_type=jnp.float32)
    carry = jnp.zeros((clusters, LANES), jnp.float32)
    ranks = []
    for b in range(blocks):
        part = prefix[b * clusters:(b + 1) * clusters]
        mine = member_f[:, b * LANES:(b + 1) * LANES]
        ranks.append(jnp.sum(mine * (part[:, :LANES] + carry), axis=0, keepdims=True))
        carry = carry + part[:, LANES:]
    rank = jnp.concatenate(ranks, axis=1).astype(jnp.int32)
    me = lax.axis_index("docs") * lax.axis_size("rep") + lax.axis_index("rep")
    lane_ref[...] = rank + (me % (LANES // depth)) * depth

    rank_hot = (
        lax.broadcasted_iota(jnp.int32, (LANES, n_rows), 0) % depth == rank
    ).astype(jnp.float32).astype(jnp.bfloat16)
    order = total - index_ref[...]
    digit_id = lax.broadcasted_iota(jnp.int32, (extra, n_rows), 0)
    digits = jnp.zeros((extra, n_rows), jnp.float32)
    left, digit = total, 0
    while left > 0:
        value = ((order >> (8 * digit)) & (BASE - 1)).astype(jnp.float32)
        digits = jnp.where(digit_id == digit, value, digits)
        left, digit = left // BASE, digit + 1
    masked = jnp.concatenate(
        [jnp.where(cluster == c, digits, 0.0) for c in range(clusters)], axis=0
    ).astype(jnp.bfloat16)
    coded = nt_dot(masked, rank_hot).astype(jnp.bfloat16)
    for c in range(clusters):
        send_ref[c, 2 * depth:, :] = coded[c * extra:(c + 1) * extra, :]

    seat = lax.broadcasted_iota(jnp.int32, (depth, n_rows), 0).astype(jnp.float32).astype(jnp.bfloat16)
    one = jnp.ones((depth, n_rows), jnp.bfloat16)
    none = jnp.zeros((depth, n_rows), jnp.bfloat16)
    for c in range(clusters):
        here = jnp.where(cluster == c, rank.astype(jnp.float32), -1.0).astype(jnp.bfloat16)
        place[c * depth:(c + 1) * depth, :] = jnp.where(seat == here, one, none)

    basis_copy.wait()
    size = 256
    for k in range(n_rows // size):
        if k * size == 0:
            for q in range(FIRST):
                emb_copy(q).wait()
        if k * size == FIRST * step:
            for q in range(FIRST, CHUNKS):
                emb_copy(q).wait()
        part = slice(k * size, (k + 1) * size)
        projected = jnp.dot(emb[part, :], basis[...], preferred_element_type=jnp.float32)
        scale = lax.rsqrt(jnp.sum(projected * projected, axis=1, keepdims=True) + 1e-06)
        rows[part, :] = (projected * scale).astype(jnp.bfloat16)
    packed = jnp.dot(place[...], rows[...], preferred_element_type=jnp.float32).astype(jnp.bfloat16)
    send_ref[:, :depth, :] = packed[:, :LANES].reshape(clusters, depth, LANES)
    send_ref[:, depth:2 * depth, :] = packed[:, LANES:].reshape(clusters, depth, LANES)


def nearest_kernel(recv_rows, out_ref, x, col, side, *, depth):
    n, groups = recv_rows.shape[:2]
    recv_ref = recv_rows.reshape(n, groups * ROWS, LANES)
    extra = groups * ROWS - 2 * depth
    slots = n * depth
    group = LANES // depth
    x[:, :LANES] = recv_ref[:, :depth, :].reshape(slots, LANES)
    x[:, LANES:] = recv_ref[:, depth:2 * depth, :].reshape(slots, LANES)
    digit_id = lax.broadcasted_iota(jnp.int32, (n, extra, LANES), 1)
    weight = jnp.where(
        digit_id == 0, 1.0, jnp.where(digit_id == 1, float(BASE), float(BASE * BASE))
    )
    digits = recv_ref[:, 2 * depth:, :].astype(jnp.float32)
    order = jnp.sum(digits * weight, axis=1)
    lane_group = lax.broadcasted_iota(jnp.int32, (1, LANES), 1) // depth
    rows_of = []
    for k in range(slots // LANES):
        row = order[k * group:k * group + 1, :]
        for q in range(1, group):
            row = jnp.where(lane_group == q, order[k * group + q:k * group + q + 1, :], row)
        rows_of.append(row)
    turned = order.T
    for c in range(n):
        col[c * depth:(c + 1) * depth, :] = jnp.broadcast_to(
            turned[:depth, c:c + 1], (depth, LANES)
        )
    tile = 256
    tiles = slots // tile
    tops = {}
    for i in range(tiles):
        right = x[i * tile:(i + 1) * tile, :]
        best = [jnp.full((8, LANES), -1.0, jnp.float32) for _ in range(2)]
        for j in range(i + 1):
            scores = nt_dot(x[j * tile:(j + 1) * tile, :], right)
            part = slice(j * tile, (j + 1) * tile)
            here = col[part, :]
            mirrored = None
            for h in range(2):
                mine = scores[:, h * LANES:(h + 1) * LANES]
                before = here > rows_of[2 * i + h]
                kept = jnp.where(before, mine, -1.0)
                best[h] = jnp.maximum(best[h], jnp.max(kept.reshape(tile // 8, 8, LANES), axis=0))
                if j < i:
                    other = jnp.where(before, -1.0, mine)
                    mirrored = other if mirrored is None else jnp.maximum(mirrored, other)
            if j < i:
                if i > j + 1:
                    mirrored = jnp.maximum(mirrored, side[part, :])
                if i < tiles - 1:
                    side[part, :] = mirrored
                else:
                    for h in range(2):
                        turned_side = mirrored[h * LANES:(h + 1) * LANES, :].T
                        tops[2 * j + h] = jnp.maximum(
                            tops[2 * j + h], jnp.max(turned_side, axis=0, keepdims=True)
                        )
        for h in range(2):
            tops[2 * i + h] = jnp.max(best[h], axis=0, keepdims=True)
    for k in range(slots // LANES):
        for q in range(group):
            out_ref[k * group + q] = tops[k]


def collect_kernel(back_ref, cluster_ref, lane_ref, out_ref):
    n = back_ref.shape[0]
    n_rows = cluster_ref.shape[1]
    back = back_ref[...].reshape(n, LANES)
    high = back.astype(jnp.bfloat16)
    rest = back - high.astype(jnp.float32)
    middle = rest.astype(jnp.bfloat16)
    low = (rest - middle.astype(jnp.float32)).astype(jnp.bfloat16)
    hot = (
        lax.broadcasted_iota(jnp.int32, (LANES, n_rows), 0) == lane_ref[...]
    ).astype(jnp.float32).astype(jnp.bfloat16)
    picked = jnp.dot(high, hot, preferred_element_type=jnp.float32)
    picked = picked + jnp.dot(middle, hot, preferred_element_type=jnp.float32)
    picked = picked + jnp.dot(low, hot, preferred_element_type=jnp.float32)
    mine = lax.broadcasted_iota(jnp.int32, (n, n_rows), 0) == cluster_ref[...]
    out_ref[...] = jnp.sum(jnp.where(mine, picked, 0.0), axis=0, keepdims=True)


def on_device(embeddings, pca_basis, cluster, doc_index):
    n_docs = lax.axis_size("docs")
    n_rep = lax.axis_size("rep")
    n_dev = n_docs * n_rep
    doc_rows, width = embeddings.shape
    features = pca_basis.shape[1]
    clusters = CL_DEV * n_docs
    assert clusters == n_dev and features == 2 * LANES
    depth = max(2, 2 * doc_rows // clusters)
    cluster_row = cluster.reshape(1, doc_rows)
    index_row = doc_index.reshape(1, doc_rows)
    vmem = pl.BlockSpec(memory_space=pltpu.VMEM)
    hbm = pl.BlockSpec(memory_space=pltpu.HBM)
    message = 2 * depth + extra_rows(doc_rows * n_dev)

    def pack(*refs):
        project_and_pack(*refs, depth=depth, clusters=clusters, total=doc_rows * n_dev)

    send, lane = pl.pallas_call(
        pack,
        name="project_and_pack",
        compiler_params=pltpu.CompilerParams(vmem_limit_bytes=28 * 2**20),
        in_specs=[hbm, hbm, hbm, hbm],
        out_specs=[vmem, vmem],
        out_shape=[
            jax.ShapeDtypeStruct((n_dev, message // ROWS, ROWS, LANES), jnp.bfloat16),
            jax.ShapeDtypeStruct((1, doc_rows), jnp.int32),
        ],
        scratch_shapes=[
            pltpu.VMEM((1, doc_rows), jnp.int32),
            pltpu.VMEM((1, doc_rows), jnp.int32),
            pltpu.VMEM((doc_rows, width), jnp.bfloat16),
            pltpu.VMEM((width, features), jnp.bfloat16),
            pltpu.VMEM((doc_rows, features), jnp.bfloat16),
            pltpu.VMEM((clusters * depth, doc_rows), jnp.bfloat16),
            pltpu.SemaphoreType.DMA((CHUNKS,)),
            pltpu.SemaphoreType.DMA,
            pltpu.SemaphoreType.DMA((2,)),
        ],
    )(*[pltpu.with_memory_space_constraint(a, pltpu.HBM) for a in (cluster_row, index_row, embeddings, pca_basis)])
    recv = lax.all_to_all(send, AXES, split_axis=0, concat_axis=0, tiled=True)

    def search(*refs):
        nearest_kernel(*refs, depth=depth)

    found = pl.pallas_call(
        search,
        name="nearest",
        compiler_params=pltpu.CompilerParams(vmem_limit_bytes=16 * 2**20),
        in_specs=[vmem],
        out_specs=vmem,
        out_shape=jax.ShapeDtypeStruct((n_dev, 1, LANES), jnp.float32),
        scratch_shapes=[
            pltpu.VMEM((n_dev * depth, features), jnp.bfloat16),
            pltpu.VMEM((n_dev * depth, LANES), jnp.float32),
            pltpu.VMEM((n_dev * depth, LANES), jnp.float32),
        ],
    )(recv)
    back = lax.all_to_all(found, AXES, split_axis=0, concat_axis=0, tiled=True)
    nearest = pl.pallas_call(
        collect_kernel,
        name="collect",
        compiler_params=pltpu.CompilerParams(vmem_limit_bytes=8 * 2**20),
        in_specs=[vmem, vmem, vmem],
        out_specs=vmem,
        out_shape=jax.ShapeDtypeStruct((1, doc_rows), jnp.float32),
    )(back, cluster_row, lane)
    return nearest.reshape(doc_rows)


def solution(mesh):
    return jax.shard_map(
        on_device,
        mesh=mesh,
        in_specs=(P(AXES, None), P(), P(AXES, None), P(AXES)),
        out_specs=P(AXES),
        check_vma=False,
    )
```

```python
import jax
import jax.numpy as jnp
from jax import lax
from jax.experimental import pallas as pl
from jax.experimental.pallas import tpu as pltpu
from jax.sharding import PartitionSpec as P

CL_DEV = 4
AXES = ("docs", "rep")
LANES = 128
ROWS = 4
CHUNKS = 8
FIRST = 4
BASE = 256


def extra_rows(total):
    digits = 1
    while BASE ** digits <= total:
        digits += 1
    return -(-digits // ROWS) * ROWS


def nt_dot(a, b):
    return lax.dot_general(a, b, (((1,), (1,)), ((), ())), preferred_element_type=jnp.float32)


def project_and_pack(
    cluster_hbm, index_hbm, emb_hbm, basis_hbm, send_rows, lane_ref,
    cluster_ref, index_ref, emb, basis, rows, place, emb_sem, basis_sem, id_sem, *, depth, clusters, total,
):
    extra = extra_rows(total)
    send_ref = send_rows.reshape(clusters, 2 * depth + extra, LANES)
    n_rows, width = emb.shape
    features = basis.shape[1]
    step = n_rows // CHUNKS

    def emb_copy(k):
        part = pl.ds(k * step, step)
        return pltpu.make_async_copy(emb_hbm.at[part], emb.at[part], emb_sem.at[k])

    cluster_copy = pltpu.make_async_copy(cluster_hbm, cluster_ref, id_sem.at[0])
    index_copy = pltpu.make_async_copy(index_hbm, index_ref, id_sem.at[1])
    cluster_copy.start()
    index_copy.start()
    basis_copy = pltpu.make_async_copy(basis_hbm, basis, basis_sem)
    basis_copy.start()
    for k in range(CHUNKS):
        emb_copy(k).start(priority=0 if k < FIRST else 1)

    cluster_copy.wait()
    index_copy.wait()
    cluster = cluster_ref[...]
    blocks = n_rows // LANES
    cluster_iota = lax.broadcasted_iota(jnp.int32, (clusters, n_rows), 0)
    member = cluster_iota == cluster
    member_f = member.astype(jnp.float32)
    stacked = jnp.concatenate(
        [member_f[:, b * LANES:(b + 1) * LANES] for b in range(blocks)], axis=0
    ).astype(jnp.bfloat16)
    row_id = lax.broadcasted_iota(jnp.int32, (LANES, 2 * LANES), 0)
    col_id = lax.broadcasted_iota(jnp.int32, (LANES, 2 * LANES), 1)
    earlier = ((row_id < col_id) | (col_id >= LANES)).astype(jnp.float32).astype(jnp.bfloat16)
    prefix = jnp.dot(stacked, earlier, preferred_element_type=jnp.float32)
    carry = jnp.zeros((clusters, LANES), jnp.float32)
    ranks = []
    for b in range(blocks):
        part = prefix[b * clusters:(b + 1) * clusters]
        mine = member_f[:, b * LANES:(b + 1) * LANES]
        ranks.append(jnp.sum(mine * (part[:, :LANES] + carry), axis=0, keepdims=True))
        carry = carry + part[:, LANES:]
    rank = jnp.concatenate(ranks, axis=1).astype(jnp.int32)
    me = lax.axis_index("docs") * lax.axis_size("rep") + lax.axis_index("rep")
    lane_ref[...] = rank + (me % (LANES // depth)) * depth

    rank_hot = (
        lax.broadcasted_iota(jnp.int32, (LANES, n_rows), 0) % depth == rank
    ).astype(jnp.float32).astype(jnp.bfloat16)
    order = total - index_ref[...]
    digit_id = lax.broadcasted_iota(jnp.int32, (extra, n_rows), 0)
    digits = jnp.zeros((extra, n_rows), jnp.float32)
    left, digit = total, 0
    while left > 0:
        value = ((order >> (8 * digit)) & (BASE - 1)).astype(jnp.float32)
        digits = jnp.where(digit_id == digit, value, digits)
        left, digit = left // BASE, digit + 1
    masked = jnp.concatenate(
        [jnp.where(cluster == c, digits, 0.0) for c in range(clusters)], axis=0
    ).astype(jnp.bfloat16)
    coded = nt_dot(masked, rank_hot).astype(jnp.bfloat16)
    for c in range(clusters):
        send_ref[c, 2 * depth:, :] = coded[c * extra:(c + 1) * extra, :]

    seat = lax.broadcasted_iota(jnp.int32, (depth, n_rows), 0).astype(jnp.float32).astype(jnp.bfloat16)
    one = jnp.ones((depth, n_rows), jnp.bfloat16)
    none = jnp.zeros((depth, n_rows), jnp.bfloat16)
    for c in range(clusters):
        here = jnp.where(cluster == c, rank.astype(jnp.float32), -1.0).astype(jnp.bfloat16)
        place[c * depth:(c + 1) * depth, :] = jnp.where(seat == here, one, none)

    basis_copy.wait()
    size = 256
    for k in range(n_rows // size):
        if k * size == 0:
            for q in range(FIRST):
                emb_copy(q).wait()
        if k * size == FIRST * step:
            for q in range(FIRST, CHUNKS):
                emb_copy(q).wait()
        part = slice(k * size, (k + 1) * size)
        projected = jnp.dot(emb[part, :], basis[...], preferred_element_type=jnp.float32)
        scale = lax.rsqrt(jnp.sum(projected * projected, axis=1, keepdims=True) + 1e-06)
        rows[part, :] = (projected * scale).astype(jnp.bfloat16)
    tall = min(512, clusters * depth)
    per = tall // depth
    for t in range(clusters // per):
        packed = jnp.dot(
            place[t * tall:(t + 1) * tall, :], rows[...], preferred_element_type=jnp.float32
        ).astype(jnp.bfloat16)
        some = slice(t * per, (t + 1) * per)
        send_ref[some, :depth, :] = packed[:, :LANES].reshape(per, depth, LANES)
        send_ref[some, depth:2 * depth, :] = packed[:, LANES:].reshape(per, depth, LANES)


def nearest_kernel(recv_rows, out_ref, x, col, side, *, depth):
    n, groups = recv_rows.shape[:2]
    recv_ref = recv_rows.reshape(n, groups * ROWS, LANES)
    extra = groups * ROWS - 2 * depth
    slots = n * depth
    group = LANES // depth
    x[:, :LANES] = recv_ref[:, :depth, :].reshape(slots, LANES)
    x[:, LANES:] = recv_ref[:, depth:2 * depth, :].reshape(slots, LANES)
    digit_id = lax.broadcasted_iota(jnp.int32, (n, extra, LANES), 1)
    weight = jnp.where(
        digit_id == 0, 1.0, jnp.where(digit_id == 1, float(BASE), float(BASE * BASE))
    )
    digits = recv_ref[:, 2 * depth:, :].astype(jnp.float32)
    order = jnp.sum(digits * weight, axis=1)
    lane_group = lax.broadcasted_iota(jnp.int32, (1, LANES), 1) // depth
    rows_of = []
    for k in range(slots // LANES):
        row = order[k * group:k * group + 1, :]
        for q in range(1, group):
            row = jnp.where(lane_group == q, order[k * group + q:k * group + q + 1, :], row)
        rows_of.append(row)
    turned = order.T
    for c in range(n):
        col[c * depth:(c + 1) * depth, :] = jnp.broadcast_to(
            turned[:depth, c:c + 1], (depth, LANES)
        )
    tile = 256
    tiles = slots // tile
    tops = {}
    for i in range(tiles):
        right = x[i * tile:(i + 1) * tile, :]
        best = [jnp.full((8, LANES), -1.0, jnp.float32) for _ in range(2)]
        for j in range(i + 1):
            scores = nt_dot(x[j * tile:(j + 1) * tile, :], right)
            part = slice(j * tile, (j + 1) * tile)
            here = col[part, :]
            mirrored = None
            for h in range(2):
                mine = scores[:, h * LANES:(h + 1) * LANES]
                before = here > rows_of[2 * i + h]
                kept = jnp.where(before, mine, -1.0)
                best[h] = jnp.maximum(best[h], jnp.max(kept.reshape(tile // 8, 8, LANES), axis=0))
                if j < i:
                    other = jnp.where(before, -1.0, mine)
                    mirrored = other if mirrored is None else jnp.maximum(mirrored, other)
            if j < i:
                if i > j + 1:
                    mirrored = jnp.maximum(mirrored, side[part, :])
                if i < tiles - 1:
                    side[part, :] = mirrored
                else:
                    for h in range(2):
                        turned_side = mirrored[h * LANES:(h + 1) * LANES, :].T
                        tops[2 * j + h] = jnp.maximum(
                            tops[2 * j + h], jnp.max(turned_side, axis=0, keepdims=True)
                        )
        for h in range(2):
            tops[2 * i + h] = jnp.max(best[h], axis=0, keepdims=True)
    for k in range(slots // LANES):
        for q in range(group):
            out_ref[k * group + q] = tops[k]


def collect_kernel(back_ref, cluster_ref, lane_ref, out_ref):
    n = back_ref.shape[0]
    n_rows = cluster_ref.shape[1]
    back = back_ref[...].reshape(n, LANES)
    high = back.astype(jnp.bfloat16)
    rest = back - high.astype(jnp.float32)
    middle = rest.astype(jnp.bfloat16)
    low = (rest - middle.astype(jnp.float32)).astype(jnp.bfloat16)
    hot = (
        lax.broadcasted_iota(jnp.int32, (LANES, n_rows), 0) == lane_ref[...]
    ).astype(jnp.float32).astype(jnp.bfloat16)
    parts = jnp.dot(
        jnp.concatenate([high, middle, low], axis=0), hot, preferred_element_type=jnp.float32
    )
    picked = parts[:n] + parts[n:2 * n] + parts[2 * n:]
    mine = lax.broadcasted_iota(jnp.int32, (n, n_rows), 0) == cluster_ref[...]
    out_ref[...] = jnp.sum(jnp.where(mine, picked, 0.0), axis=0, keepdims=True)


def on_device(embeddings, pca_basis, cluster, doc_index):
    n_docs = lax.axis_size("docs")
    n_rep = lax.axis_size("rep")
    n_dev = n_docs * n_rep
    doc_rows, width = embeddings.shape
    features = pca_basis.shape[1]
    clusters = CL_DEV * n_docs
    assert clusters == n_dev and features == 2 * LANES
    depth = max(2, 2 * doc_rows // clusters)
    cluster_row = cluster.reshape(1, doc_rows)
    index_row = doc_index.reshape(1, doc_rows)
    vmem = pl.BlockSpec(memory_space=pltpu.VMEM)
    hbm = pl.BlockSpec(memory_space=pltpu.HBM)
    message = 2 * depth + extra_rows(doc_rows * n_dev)

    def pack(*refs):
        project_and_pack(*refs, depth=depth, clusters=clusters, total=doc_rows * n_dev)

    send, lane = pl.pallas_call(
        pack,
        name="project_and_pack",
        compiler_params=pltpu.CompilerParams(vmem_limit_bytes=28 * 2**20),
        in_specs=[hbm, hbm, hbm, hbm],
        out_specs=[vmem, vmem],
        out_shape=[
            jax.ShapeDtypeStruct((n_dev, message // ROWS, ROWS, LANES), jnp.bfloat16),
            jax.ShapeDtypeStruct((1, doc_rows), jnp.int32),
        ],
        scratch_shapes=[
            pltpu.VMEM((1, doc_rows), jnp.int32),
            pltpu.VMEM((1, doc_rows), jnp.int32),
            pltpu.VMEM((doc_rows, width), jnp.bfloat16),
            pltpu.VMEM((width, features), jnp.bfloat16),
            pltpu.VMEM((doc_rows, features), jnp.bfloat16),
            pltpu.VMEM((clusters * depth, doc_rows), jnp.bfloat16),
            pltpu.SemaphoreType.DMA((CHUNKS,)),
            pltpu.SemaphoreType.DMA,
            pltpu.SemaphoreType.DMA((2,)),
        ],
    )(*[pltpu.with_memory_space_constraint(a, pltpu.HBM) for a in (cluster_row, index_row, embeddings, pca_basis)])
    recv = lax.all_to_all(send, AXES, split_axis=0, concat_axis=0, tiled=True)

    def search(*refs):
        nearest_kernel(*refs, depth=depth)

    found = pl.pallas_call(
        search,
        name="nearest",
        compiler_params=pltpu.CompilerParams(vmem_limit_bytes=16 * 2**20),
        in_specs=[vmem],
        out_specs=vmem,
        out_shape=jax.ShapeDtypeStruct((n_dev, 1, LANES), jnp.float32),
        scratch_shapes=[
            pltpu.VMEM((n_dev * depth, features), jnp.bfloat16),
            pltpu.VMEM((n_dev * depth, LANES), jnp.float32),
            pltpu.VMEM((n_dev * depth, LANES), jnp.float32),
        ],
    )(recv)
    back = lax.all_to_all(found, AXES, split_axis=0, concat_axis=0, tiled=True)
    nearest = pl.pallas_call(
        collect_kernel,
        name="collect",
        compiler_params=pltpu.CompilerParams(vmem_limit_bytes=8 * 2**20),
        in_specs=[vmem, vmem, vmem],
        out_specs=vmem,
        out_shape=jax.ShapeDtypeStruct((1, doc_rows), jnp.float32),
    )(back, cluster_row, lane)
    return nearest.reshape(doc_rows)


def solution(mesh):
    return jax.shard_map(
        on_device,
        mesh=mesh,
        in_specs=(P(AXES, None), P(), P(AXES, None), P(AXES)),
        out_specs=P(AXES),
        check_vma=False,
    )
```

```python
import jax
import jax.numpy as jnp
from jax import lax
from jax.experimental import pallas as pl
from jax.experimental.pallas import tpu as pltpu
from jax.sharding import PartitionSpec as P

CL_DEV = 4
AXES = ("docs", "rep")
LANES = 128
ROWS = 4
CHUNKS = 2
BASE = 256


def extra_rows(total):
    digits = 1
    while BASE ** digits <= total:
        digits += 1
    return -(-digits // ROWS) * ROWS


def nt_dot(a, b):
    return lax.dot_general(a, b, (((1,), (1,)), ((), ())), preferred_element_type=jnp.float32)


def project_and_pack(
    cluster_hbm, index_hbm, emb_hbm, basis_hbm, send_rows, lane_ref,
    cluster_ref, index_ref, emb, basis, partial, rows, place, emb_sem, basis_sem, id_sem, *, depth, clusters, total,
):
    extra = extra_rows(total)
    send_ref = send_rows.reshape(clusters, 2 * depth + extra, LANES)
    n_rows, width = emb.shape
    features = basis.shape[1]
    step = n_rows // CHUNKS

    split = width * 1 // 2
    spans = [slice(0, split), slice(split, width)]

    def basis_copy(h):
        part = pl.ds(spans[h].start, spans[h].stop - spans[h].start)
        return pltpu.make_async_copy(basis_hbm.at[part], basis.at[part], basis_sem.at[h])

    def emb_copy(h, k):
        part = pl.ds(k * step, step)
        cols = pl.ds(spans[h].start, spans[h].stop - spans[h].start)
        return pltpu.make_async_copy(
            emb_hbm.at[part, cols], emb.at[part, cols], emb_sem.at[h, k]
        )

    cluster_copy = pltpu.make_async_copy(cluster_hbm, cluster_ref, id_sem.at[0])
    index_copy = pltpu.make_async_copy(index_hbm, index_ref, id_sem.at[1])
    cluster_copy.start()
    index_copy.start()
    for h in range(2):
        basis_copy(h).start(priority=h)
        for k in range(CHUNKS):
            emb_copy(h, k).start(priority=h)

    cluster_copy.wait()
    index_copy.wait()
    cluster = cluster_ref[...]
    blocks = n_rows // LANES
    cluster_iota = lax.broadcasted_iota(jnp.int32, (clusters, n_rows), 0)
    member = cluster_iota == cluster
    member_f = member.astype(jnp.float32)
    stacked = jnp.concatenate(
        [member_f[:, b * LANES:(b + 1) * LANES] for b in range(blocks)], axis=0
    ).astype(jnp.bfloat16)
    row_id = lax.broadcasted_iota(jnp.int32, (LANES, 2 * LANES), 0)
    col_id = lax.broadcasted_iota(jnp.int32, (LANES, 2 * LANES), 1)
    earlier = ((row_id < col_id) | (col_id >= LANES)).astype(jnp.float32).astype(jnp.bfloat16)
    prefix = jnp.dot(stacked, earlier, preferred_element_type=jnp.float32)
    carry = jnp.zeros((clusters, LANES), jnp.float32)
    ranks = []
    for b in range(blocks):
        part = prefix[b * clusters:(b + 1) * clusters]
        mine = member_f[:, b * LANES:(b + 1) * LANES]
        ranks.append(jnp.sum(mine * (part[:, :LANES] + carry), axis=0, keepdims=True))
        carry = carry + part[:, LANES:]
    rank = jnp.concatenate(ranks, axis=1).astype(jnp.int32)
    me = lax.axis_index("docs") * lax.axis_size("rep") + lax.axis_index("rep")
    lane_ref[...] = rank + (me % (LANES // depth)) * depth

    rank_hot = (
        lax.broadcasted_iota(jnp.int32, (LANES, n_rows), 0) % depth == rank
    ).astype(jnp.float32).astype(jnp.bfloat16)
    order = total - index_ref[...]
    digit_id = lax.broadcasted_iota(jnp.int32, (extra, n_rows), 0)
    digits = jnp.zeros((extra, n_rows), jnp.float32)
    left, digit = total, 0
    while left > 0:
        value = ((order >> (8 * digit)) & (BASE - 1)).astype(jnp.float32)
        digits = jnp.where(digit_id == digit, value, digits)
        left, digit = left // BASE, digit + 1
    masked = jnp.concatenate(
        [jnp.where(cluster == c, digits, 0.0) for c in range(clusters)], axis=0
    ).astype(jnp.bfloat16)
    coded = nt_dot(masked, rank_hot).astype(jnp.bfloat16)
    for c in range(clusters):
        send_ref[c, 2 * depth:, :] = coded[c * extra:(c + 1) * extra, :]

    seat = lax.broadcasted_iota(jnp.int32, (depth, n_rows), 0).astype(jnp.float32).astype(jnp.bfloat16)
    one = jnp.ones((depth, n_rows), jnp.bfloat16)
    none = jnp.zeros((depth, n_rows), jnp.bfloat16)
    for c in range(clusters):
        here = jnp.where(cluster == c, rank.astype(jnp.float32), -1.0).astype(jnp.bfloat16)
        place[c * depth:(c + 1) * depth, :] = jnp.where(seat == here, one, none)

    size = 256
    for h in range(2):
        basis_copy(h).wait()
        for k in range(CHUNKS):
            emb_copy(h, k).wait()
        for k in range(n_rows // size):
            part = slice(k * size, (k + 1) * size)
            projected = jnp.dot(
                emb[part, spans[h]], basis[spans[h], :], preferred_element_type=jnp.float32
            )
            if h == 0:
                partial[part, :] = projected
            else:
                projected = projected + partial[part, :]
                scale = lax.rsqrt(jnp.sum(projected * projected, axis=1, keepdims=True) + 1e-06)
                rows[part, :] = (projected * scale).astype(jnp.bfloat16)
    tall = min(512, clusters * depth)
    per = tall // depth
    for t in range(clusters // per):
        packed = jnp.dot(
            place[t * tall:(t + 1) * tall, :], rows[...], preferred_element_type=jnp.float32
        ).astype(jnp.bfloat16)
        some = slice(t * per, (t + 1) * per)
        send_ref[some, :depth, :] = packed[:, :LANES].reshape(per, depth, LANES)
        send_ref[some, depth:2 * depth, :] = packed[:, LANES:].reshape(per, depth, LANES)


def nearest_kernel(recv_rows, out_ref, x, col, side, *, depth):
    n, groups = recv_rows.shape[:2]
    recv_ref = recv_rows.reshape(n, groups * ROWS, LANES)
    extra = groups * ROWS - 2 * depth
    slots = n * depth
    group = LANES // depth
    x[:, :LANES] = recv_ref[:, :depth, :].reshape(slots, LANES)
    x[:, LANES:] = recv_ref[:, depth:2 * depth, :].reshape(slots, LANES)
    digit_id = lax.broadcasted_iota(jnp.int32, (n, extra, LANES), 1)
    weight = jnp.where(
        digit_id == 0, 1.0, jnp.where(digit_id == 1, float(BASE), float(BASE * BASE))
    )
    digits = recv_ref[:, 2 * depth:, :].astype(jnp.float32)
    order = jnp.sum(digits * weight, axis=1)
    lane_group = lax.broadcasted_iota(jnp.int32, (1, LANES), 1) // depth
    rows_of = []
    for k in range(slots // LANES):
        row = order[k * group:k * group + 1, :]
        for q in range(1, group):
            row = jnp.where(lane_group == q, order[k * group + q:k * group + q + 1, :], row)
        rows_of.append(row)
    turned = order.T
    for c in range(n):
        col[c * depth:(c + 1) * depth, :] = jnp.broadcast_to(
            turned[:depth, c:c + 1], (depth, LANES)
        )
    tile = 256
    tiles = slots // tile
    tops = {}
    for i in range(tiles):
        right = x[i * tile:(i + 1) * tile, :]
        best = [jnp.full((8, LANES), -1.0, jnp.float32) for _ in range(2)]
        for j in range(i + 1):
            scores = nt_dot(x[j * tile:(j + 1) * tile, :], right)
            part = slice(j * tile, (j + 1) * tile)
            here = col[part, :]
            mirrored = None
            for h in range(2):
                mine = scores[:, h * LANES:(h + 1) * LANES]
                before = here > rows_of[2 * i + h]
                kept = jnp.where(before, mine, -1.0)
                best[h] = jnp.maximum(best[h], jnp.max(kept.reshape(tile // 8, 8, LANES), axis=0))
                if j < i:
                    other = jnp.where(before, -1.0, mine)
                    mirrored = other if mirrored is None else jnp.maximum(mirrored, other)
            if j < i:
                if i > j + 1:
                    mirrored = jnp.maximum(mirrored, side[part, :])
                if i < tiles - 1:
                    side[part, :] = mirrored
                else:
                    for h in range(2):
                        turned_side = mirrored[h * LANES:(h + 1) * LANES, :].T
                        tops[2 * j + h] = jnp.maximum(
                            tops[2 * j + h], jnp.max(turned_side, axis=0, keepdims=True)
                        )
        for h in range(2):
            tops[2 * i + h] = jnp.max(best[h], axis=0, keepdims=True)
    for k in range(slots // LANES):
        for q in range(group):
            out_ref[k * group + q] = tops[k]


def collect_kernel(back_ref, cluster_ref, lane_ref, out_ref):
    n = back_ref.shape[0]
    n_rows = cluster_ref.shape[1]
    back = back_ref[...].reshape(n, LANES)
    high = back.astype(jnp.bfloat16)
    rest = back - high.astype(jnp.float32)
    middle = rest.astype(jnp.bfloat16)
    low = (rest - middle.astype(jnp.float32)).astype(jnp.bfloat16)
    hot = (
        lax.broadcasted_iota(jnp.int32, (LANES, n_rows), 0) == lane_ref[...]
    ).astype(jnp.float32).astype(jnp.bfloat16)
    parts = jnp.dot(
        jnp.concatenate([high, middle, low], axis=0), hot, preferred_element_type=jnp.float32
    )
    picked = parts[:n] + parts[n:2 * n] + parts[2 * n:]
    mine = lax.broadcasted_iota(jnp.int32, (n, n_rows), 0) == cluster_ref[...]
    out_ref[...] = jnp.sum(jnp.where(mine, picked, 0.0), axis=0, keepdims=True)


def on_device(embeddings, pca_basis, cluster, doc_index):
    n_docs = lax.axis_size("docs")
    n_rep = lax.axis_size("rep")
    n_dev = n_docs * n_rep
    doc_rows, width = embeddings.shape
    features = pca_basis.shape[1]
    clusters = CL_DEV * n_docs
    assert clusters == n_dev and features == 2 * LANES
    depth = max(2, 2 * doc_rows // clusters)
    cluster_row = cluster.reshape(1, doc_rows)
    index_row = doc_index.reshape(1, doc_rows)
    vmem = pl.BlockSpec(memory_space=pltpu.VMEM)
    hbm = pl.BlockSpec(memory_space=pltpu.HBM)
    message = 2 * depth + extra_rows(doc_rows * n_dev)

    def pack(*refs):
        project_and_pack(*refs, depth=depth, clusters=clusters, total=doc_rows * n_dev)

    send, lane = pl.pallas_call(
        pack,
        name="project_and_pack",
        compiler_params=pltpu.CompilerParams(vmem_limit_bytes=28 * 2**20),
        in_specs=[hbm, hbm, hbm, hbm],
        out_specs=[vmem, vmem],
        out_shape=[
            jax.ShapeDtypeStruct((n_dev, message // ROWS, ROWS, LANES), jnp.bfloat16),
            jax.ShapeDtypeStruct((1, doc_rows), jnp.int32),
        ],
        scratch_shapes=[
            pltpu.VMEM((1, doc_rows), jnp.int32),
            pltpu.VMEM((1, doc_rows), jnp.int32),
            pltpu.VMEM((doc_rows, width), jnp.bfloat16),
            pltpu.VMEM((width, features), jnp.bfloat16),
            pltpu.VMEM((doc_rows, features), jnp.float32),
            pltpu.VMEM((doc_rows, features), jnp.bfloat16),
            pltpu.VMEM((clusters * depth, doc_rows), jnp.bfloat16),
            pltpu.SemaphoreType.DMA((2, CHUNKS)),
            pltpu.SemaphoreType.DMA((2,)),
            pltpu.SemaphoreType.DMA((2,)),
        ],
    )(*[pltpu.with_memory_space_constraint(a, pltpu.HBM) for a in (cluster_row, index_row, embeddings, pca_basis)])
    recv = lax.all_to_all(send, AXES, split_axis=0, concat_axis=0, tiled=True)

    def search(*refs):
        nearest_kernel(*refs, depth=depth)

    found = pl.pallas_call(
        search,
        name="nearest",
        compiler_params=pltpu.CompilerParams(vmem_limit_bytes=16 * 2**20),
        in_specs=[vmem],
        out_specs=vmem,
        out_shape=jax.ShapeDtypeStruct((n_dev, 1, LANES), jnp.float32),
        scratch_shapes=[
            pltpu.VMEM((n_dev * depth, features), jnp.bfloat16),
            pltpu.VMEM((n_dev * depth, LANES), jnp.float32),
            pltpu.VMEM((n_dev * depth, LANES), jnp.float32),
        ],
    )(recv)
    back = lax.all_to_all(found, AXES, split_axis=0, concat_axis=0, tiled=True)
    nearest = pl.pallas_call(
        collect_kernel,
        name="collect",
        compiler_params=pltpu.CompilerParams(vmem_limit_bytes=8 * 2**20),
        in_specs=[vmem, vmem, vmem],
        out_specs=vmem,
        out_shape=jax.ShapeDtypeStruct((1, doc_rows), jnp.float32),
    )(back, cluster_row, lane)
    return nearest.reshape(doc_rows)


def solution(mesh):
    return jax.shard_map(
        on_device,
        mesh=mesh,
        in_specs=(P(AXES, None), P(), P(AXES, None), P(AXES)),
        out_specs=P(AXES),
        check_vma=False,
    )
```

```python
import jax
import jax.numpy as jnp
from jax import lax
from jax.experimental import pallas as pl
from jax.experimental.pallas import tpu as pltpu
from jax.sharding import PartitionSpec as P

CL_DEV = 4
AXES = ("docs", "rep")
LANES = 128
ROWS = 4
CHUNKS = 2
BASE = 256


def extra_rows(total):
    digits = 1
    while BASE ** digits <= total:
        digits += 1
    return -(-digits // ROWS) * ROWS


def nt_dot(a, b):
    return lax.dot_general(a, b, (((1,), (1,)), ((), ())), preferred_element_type=jnp.float32)


def project_and_pack(
    cluster_hbm, index_hbm, emb_hbm, basis_hbm, send_rows, lane_ref,
    cluster_ref, index_ref, emb, basis, partial, rows, place, emb_sem, basis_sem, id_sem, *, depth, clusters, total,
):
    extra = extra_rows(total)
    send_ref = send_rows.reshape(clusters, 2 * depth + extra, LANES)
    n_rows, width = emb.shape
    features = basis.shape[1]
    step = n_rows // CHUNKS

    split = width * 1 // 2
    spans = [slice(0, split), slice(split, width)]

    def basis_copy(h):
        part = pl.ds(spans[h].start, spans[h].stop - spans[h].start)
        return pltpu.make_async_copy(basis_hbm.at[part], basis.at[part], basis_sem.at[h])

    def emb_copy(h, k):
        part = pl.ds(k * step, step)
        cols = pl.ds(spans[h].start, spans[h].stop - spans[h].start)
        return pltpu.make_async_copy(
            emb_hbm.at[part, cols], emb.at[part, cols], emb_sem.at[h, k]
        )

    cluster_copy = pltpu.make_async_copy(cluster_hbm, cluster_ref, id_sem.at[0])
    index_copy = pltpu.make_async_copy(index_hbm, index_ref, id_sem.at[1])
    cluster_copy.start()
    index_copy.start()
    for h in range(2):
        basis_copy(h).start(priority=h)
        for k in range(CHUNKS):
            emb_copy(h, k).start(priority=h)

    cluster_copy.wait()
    index_copy.wait()
    cluster = cluster_ref[...]
    blocks = n_rows // LANES
    cluster_iota = lax.broadcasted_iota(jnp.int32, (clusters, n_rows), 0)
    member = cluster_iota == cluster
    member_f = member.astype(jnp.float32)
    stacked = jnp.concatenate(
        [member_f[:, b * LANES:(b + 1) * LANES] for b in range(blocks)], axis=0
    ).astype(jnp.bfloat16)
    row_id = lax.broadcasted_iota(jnp.int32, (LANES, 2 * LANES), 0)
    col_id = lax.broadcasted_iota(jnp.int32, (LANES, 2 * LANES), 1)
    earlier = ((row_id < col_id) | (col_id >= LANES)).astype(jnp.float32).astype(jnp.bfloat16)
    prefix = jnp.dot(stacked, earlier, preferred_element_type=jnp.float32)
    carry = jnp.zeros((clusters, LANES), jnp.float32)
    ranks = []
    for b in range(blocks):
        part = prefix[b * clusters:(b + 1) * clusters]
        mine = member_f[:, b * LANES:(b + 1) * LANES]
        ranks.append(jnp.sum(mine * (part[:, :LANES] + carry), axis=0, keepdims=True))
        carry = carry + part[:, LANES:]
    rank = jnp.concatenate(ranks, axis=1).astype(jnp.int32)
    me = lax.axis_index("docs") * lax.axis_size("rep") + lax.axis_index("rep")
    lane_ref[...] = rank + (me % (LANES // depth)) * depth

    rank_hot = (
        lax.broadcasted_iota(jnp.int32, (LANES, n_rows), 0) % depth == rank
    ).astype(jnp.float32).astype(jnp.bfloat16)
    order = total - index_ref[...]
    digit_id = lax.broadcasted_iota(jnp.int32, (extra, n_rows), 0)
    digits = jnp.zeros((extra, n_rows), jnp.float32)
    left, digit = total, 0
    while left > 0:
        value = ((order >> (8 * digit)) & (BASE - 1)).astype(jnp.float32)
        digits = jnp.where(digit_id == digit, value, digits)
        left, digit = left // BASE, digit + 1
    masked = jnp.concatenate(
        [jnp.where(cluster == c, digits, 0.0) for c in range(clusters)], axis=0
    ).astype(jnp.bfloat16)
    coded = nt_dot(masked, rank_hot).astype(jnp.bfloat16)
    for c in range(clusters):
        send_ref[c, 2 * depth:, :] = coded[c * extra:(c + 1) * extra, :]

    seat = lax.broadcasted_iota(jnp.int32, (depth, n_rows), 0).astype(jnp.float32).astype(jnp.bfloat16)
    one = jnp.ones((depth, n_rows), jnp.bfloat16)
    none = jnp.zeros((depth, n_rows), jnp.bfloat16)
    for c in range(clusters):
        here = jnp.where(cluster == c, rank.astype(jnp.float32), -1.0).astype(jnp.bfloat16)
        place[c * depth:(c + 1) * depth, :] = jnp.where(seat == here, one, none)

    size = 256
    for h in range(2):
        basis_copy(h).wait()
        for k in range(CHUNKS):
            emb_copy(h, k).wait()
        for k in range(n_rows // size):
            part = slice(k * size, (k + 1) * size)
            projected = jnp.dot(
                emb[part, spans[h]], basis[spans[h], :], preferred_element_type=jnp.float32
            )
            if h == 0:
                partial[part, :] = projected
            else:
                projected = projected + partial[part, :]
                scale = lax.rsqrt(jnp.sum(projected * projected, axis=1, keepdims=True) + 1e-06)
                rows[part, :] = (projected * scale).astype(jnp.bfloat16)
    tall = min(512, clusters * depth)
    per = tall // depth
    for t in range(clusters // per):
        packed = jnp.dot(
            place[t * tall:(t + 1) * tall, :], rows[...], preferred_element_type=jnp.float32
        ).astype(jnp.bfloat16)
        some = slice(t * per, (t + 1) * per)
        send_ref[some, :depth, :] = packed[:, :LANES].reshape(per, depth, LANES)
        send_ref[some, depth:2 * depth, :] = packed[:, LANES:].reshape(per, depth, LANES)


def nearest_kernel(recv_rows, out_ref, x, col, side, *, depth):
    n, groups = recv_rows.shape[:2]
    recv_ref = recv_rows.reshape(n, groups * ROWS, LANES)
    extra = groups * ROWS - 2 * depth
    slots = n * depth
    group = LANES // depth
    x[:, :LANES] = recv_ref[:, :depth, :].reshape(slots, LANES)
    x[:, LANES:] = recv_ref[:, depth:2 * depth, :].reshape(slots, LANES)
    digit_id = lax.broadcasted_iota(jnp.int32, (n, extra, LANES), 1)
    weight = jnp.where(
        digit_id == 0, 1.0, jnp.where(digit_id == 1, float(BASE), float(BASE * BASE))
    )
    digits = recv_ref[:, 2 * depth:, :].astype(jnp.float32)
    order = jnp.sum(digits * weight, axis=1)
    lane_group = lax.broadcasted_iota(jnp.int32, (1, LANES), 1) // depth
    rows_of = []
    for k in range(slots // LANES):
        row = order[k * group:k * group + 1, :]
        for q in range(1, group):
            row = jnp.where(lane_group == q, order[k * group + q:k * group + q + 1, :], row)
        rows_of.append(row)
    turned = order.T
    for c in range(n):
        col[c * depth:(c + 1) * depth, :] = jnp.broadcast_to(
            turned[:depth, c:c + 1], (depth, LANES)
        )
    tile = 512
    tiles = slots // tile
    halves = tile // LANES
    tops = {}
    for i in range(tiles):
        right = x[i * tile:(i + 1) * tile, :]
        best = [jnp.full((8, LANES), -1.0, jnp.float32) for _ in range(halves)]
        for j in range(i + 1):
            scores = nt_dot(x[j * tile:(j + 1) * tile, :], right)
            part = slice(j * tile, (j + 1) * tile)
            here = col[part, :]
            mirrored = None
            for h in range(halves):
                mine = scores[:, h * LANES:(h + 1) * LANES]
                before = here > rows_of[halves * i + h]
                kept = jnp.where(before, mine, -1.0)
                best[h] = jnp.maximum(best[h], jnp.max(kept.reshape(tile // 8, 8, LANES), axis=0))
                if j < i:
                    other = jnp.where(before, -1.0, mine)
                    mirrored = other if mirrored is None else jnp.maximum(mirrored, other)
            if j < i:
                if i > j + 1:
                    mirrored = jnp.maximum(mirrored, side[part, :])
                if i < tiles - 1:
                    side[part, :] = mirrored
                else:
                    for h in range(halves):
                        turned_side = mirrored[h * LANES:(h + 1) * LANES, :].T
                        tops[halves * j + h] = jnp.maximum(
                            tops[halves * j + h], jnp.max(turned_side, axis=0, keepdims=True)
                        )
        for h in range(halves):
            tops[halves * i + h] = jnp.max(best[h], axis=0, keepdims=True)
    for k in range(slots // LANES):
        for q in range(group):
            out_ref[k * group + q] = tops[k]


def collect_kernel(back_ref, cluster_ref, lane_ref, out_ref):
    n = back_ref.shape[0]
    n_rows = cluster_ref.shape[1]
    back = back_ref[...].reshape(n, LANES)
    high = back.astype(jnp.bfloat16)
    rest = back - high.astype(jnp.float32)
    middle = rest.astype(jnp.bfloat16)
    low = (rest - middle.astype(jnp.float32)).astype(jnp.bfloat16)
    hot = (
        lax.broadcasted_iota(jnp.int32, (LANES, n_rows), 0) == lane_ref[...]
    ).astype(jnp.float32).astype(jnp.bfloat16)
    parts = jnp.dot(
        jnp.concatenate([high, middle, low], axis=0), hot, preferred_element_type=jnp.float32
    )
    picked = parts[:n] + parts[n:2 * n] + parts[2 * n:]
    mine = lax.broadcasted_iota(jnp.int32, (n, n_rows), 0) == cluster_ref[...]
    out_ref[...] = jnp.sum(jnp.where(mine, picked, 0.0), axis=0, keepdims=True)


def on_device(embeddings, pca_basis, cluster, doc_index):
    n_docs = lax.axis_size("docs")
    n_rep = lax.axis_size("rep")
    n_dev = n_docs * n_rep
    doc_rows, width = embeddings.shape
    features = pca_basis.shape[1]
    clusters = CL_DEV * n_docs
    assert clusters == n_dev and features == 2 * LANES
    depth = max(2, 2 * doc_rows // clusters)
    cluster_row = cluster.reshape(1, doc_rows)
    index_row = doc_index.reshape(1, doc_rows)
    vmem = pl.BlockSpec(memory_space=pltpu.VMEM)
    hbm = pl.BlockSpec(memory_space=pltpu.HBM)
    message = 2 * depth + extra_rows(doc_rows * n_dev)

    def pack(*refs):
        project_and_pack(*refs, depth=depth, clusters=clusters, total=doc_rows * n_dev)

    send, lane = pl.pallas_call(
        pack,
        name="project_and_pack",
        compiler_params=pltpu.CompilerParams(vmem_limit_bytes=28 * 2**20),
        in_specs=[hbm, hbm, hbm, hbm],
        out_specs=[vmem, vmem],
        out_shape=[
            jax.ShapeDtypeStruct((n_dev, message // ROWS, ROWS, LANES), jnp.bfloat16),
            jax.ShapeDtypeStruct((1, doc_rows), jnp.int32),
        ],
        scratch_shapes=[
            pltpu.VMEM((1, doc_rows), jnp.int32),
            pltpu.VMEM((1, doc_rows), jnp.int32),
            pltpu.VMEM((doc_rows, width), jnp.bfloat16),
            pltpu.VMEM((width, features), jnp.bfloat16),
            pltpu.VMEM((doc_rows, features), jnp.float32),
            pltpu.VMEM((doc_rows, features), jnp.bfloat16),
            pltpu.VMEM((clusters * depth, doc_rows), jnp.bfloat16),
            pltpu.SemaphoreType.DMA((2, CHUNKS)),
            pltpu.SemaphoreType.DMA((2,)),
            pltpu.SemaphoreType.DMA((2,)),
        ],
    )(*[pltpu.with_memory_space_constraint(a, pltpu.HBM) for a in (cluster_row, index_row, embeddings, pca_basis)])
    recv = lax.all_to_all(send, AXES, split_axis=0, concat_axis=0, tiled=True)

    def search(*refs):
        nearest_kernel(*refs, depth=depth)

    found = pl.pallas_call(
        search,
        name="nearest",
        compiler_params=pltpu.CompilerParams(vmem_limit_bytes=16 * 2**20),
        in_specs=[vmem],
        out_specs=vmem,
        out_shape=jax.ShapeDtypeStruct((n_dev, 1, LANES), jnp.float32),
        scratch_shapes=[
            pltpu.VMEM((n_dev * depth, features), jnp.bfloat16),
            pltpu.VMEM((n_dev * depth, LANES), jnp.float32),
            pltpu.VMEM((n_dev * depth, LANES), jnp.float32),
        ],
    )(recv)
    back = lax.all_to_all(found, AXES, split_axis=0, concat_axis=0, tiled=True)
    nearest = pl.pallas_call(
        collect_kernel,
        name="collect",
        compiler_params=pltpu.CompilerParams(vmem_limit_bytes=8 * 2**20),
        in_specs=[vmem, vmem, vmem],
        out_specs=vmem,
        out_shape=jax.ShapeDtypeStruct((1, doc_rows), jnp.float32),
    )(back, cluster_row, lane)
    return nearest.reshape(doc_rows)


def solution(mesh):
    return jax.shard_map(
        on_device,
        mesh=mesh,
        in_specs=(P(AXES, None), P(), P(AXES, None), P(AXES)),
        out_specs=P(AXES),
        check_vma=False,
    )
```

```python
import jax
import jax.numpy as jnp
from jax import lax
from jax.experimental import pallas as pl
from jax.experimental.pallas import tpu as pltpu
from jax.sharding import PartitionSpec as P

CL_DEV = 4
AXES = ("docs", "rep")
OWNERS = ("rep", "docs")
LANES = 128
ROWS = 4
CHUNKS = 2
BASE = 256


def extra_rows(total):
    digits = 1
    while BASE ** digits <= total:
        digits += 1
    return -(-digits // ROWS) * ROWS


def nt_dot(a, b):
    return lax.dot_general(a, b, (((1,), (1,)), ((), ())), preferred_element_type=jnp.float32)


def project_and_pack(
    cluster_hbm, index_hbm, emb_hbm, basis_hbm, send_rows, lane_ref,
    cluster_ref, index_ref, emb, basis, partial, rows, place, emb_sem, basis_sem, id_sem, *, depth, clusters, total,
):
    extra = extra_rows(total)
    send_ref = send_rows.reshape(clusters, 2 * depth + extra, LANES)
    n_rows, width = emb.shape
    features = basis.shape[1]
    step = n_rows // CHUNKS

    split = width * 1 // 2
    spans = [slice(0, split), slice(split, width)]

    def basis_copy(h):
        part = pl.ds(spans[h].start, spans[h].stop - spans[h].start)
        return pltpu.make_async_copy(basis_hbm.at[part], basis.at[part], basis_sem.at[h])

    def emb_copy(h, k):
        part = pl.ds(k * step, step)
        cols = pl.ds(spans[h].start, spans[h].stop - spans[h].start)
        return pltpu.make_async_copy(
            emb_hbm.at[part, cols], emb.at[part, cols], emb_sem.at[h, k]
        )

    cluster_copy = pltpu.make_async_copy(cluster_hbm, cluster_ref, id_sem.at[0])
    index_copy = pltpu.make_async_copy(index_hbm, index_ref, id_sem.at[1])
    cluster_copy.start()
    index_copy.start()
    for h in range(2):
        basis_copy(h).start(priority=h)
        for k in range(CHUNKS):
            emb_copy(h, k).start(priority=h)

    cluster_copy.wait()
    index_copy.wait()
    cluster = cluster_ref[...]
    blocks = n_rows // LANES
    cluster_iota = lax.broadcasted_iota(jnp.int32, (clusters, n_rows), 0)
    member = cluster_iota == cluster
    member_f = member.astype(jnp.float32)
    stacked = jnp.concatenate(
        [member_f[:, b * LANES:(b + 1) * LANES] for b in range(blocks)], axis=0
    ).astype(jnp.bfloat16)
    row_id = lax.broadcasted_iota(jnp.int32, (LANES, 2 * LANES), 0)
    col_id = lax.broadcasted_iota(jnp.int32, (LANES, 2 * LANES), 1)
    earlier = ((row_id < col_id) | (col_id >= LANES)).astype(jnp.float32).astype(jnp.bfloat16)
    prefix = jnp.dot(stacked, earlier, preferred_element_type=jnp.float32)
    carry = jnp.zeros((clusters, LANES), jnp.float32)
    ranks = []
    for b in range(blocks):
        part = prefix[b * clusters:(b + 1) * clusters]
        mine = member_f[:, b * LANES:(b + 1) * LANES]
        ranks.append(jnp.sum(mine * (part[:, :LANES] + carry), axis=0, keepdims=True))
        carry = carry + part[:, LANES:]
    rank = jnp.concatenate(ranks, axis=1).astype(jnp.int32)
    me = lax.axis_index("rep") * lax.axis_size("docs") + lax.axis_index("docs")
    lane_ref[...] = rank + (me % (LANES // depth)) * depth

    rank_hot = (
        lax.broadcasted_iota(jnp.int32, (LANES, n_rows), 0) % depth == rank
    ).astype(jnp.float32).astype(jnp.bfloat16)
    order = total - index_ref[...]
    digit_id = lax.broadcasted_iota(jnp.int32, (extra, n_rows), 0)
    digits = jnp.zeros((extra, n_rows), jnp.float32)
    left, digit = total, 0
    while left > 0:
        value = ((order >> (8 * digit)) & (BASE - 1)).astype(jnp.float32)
        digits = jnp.where(digit_id == digit, value, digits)
        left, digit = left // BASE, digit + 1
    masked = jnp.concatenate(
        [jnp.where(cluster == c, digits, 0.0) for c in range(clusters)], axis=0
    ).astype(jnp.bfloat16)
    coded = nt_dot(masked, rank_hot).astype(jnp.bfloat16)
    for c in range(clusters):
        send_ref[c, 2 * depth:, :] = coded[c * extra:(c + 1) * extra, :]

    seat = lax.broadcasted_iota(jnp.int32, (depth, n_rows), 0).astype(jnp.float32).astype(jnp.bfloat16)
    one = jnp.ones((depth, n_rows), jnp.bfloat16)
    none = jnp.zeros((depth, n_rows), jnp.bfloat16)
    for c in range(clusters):
        here = jnp.where(cluster == c, rank.astype(jnp.float32), -1.0).astype(jnp.bfloat16)
        place[c * depth:(c + 1) * depth, :] = jnp.where(seat == here, one, none)

    size = 256
    for h in range(2):
        basis_copy(h).wait()
        for k in range(CHUNKS):
            emb_copy(h, k).wait()
        for k in range(n_rows // size):
            part = slice(k * size, (k + 1) * size)
            projected = jnp.dot(
                emb[part, spans[h]], basis[spans[h], :], preferred_element_type=jnp.float32
            )
            if h == 0:
                partial[part, :] = projected
            else:
                projected = projected + partial[part, :]
                scale = lax.rsqrt(jnp.sum(projected * projected, axis=1, keepdims=True) + 1e-06)
                rows[part, :] = (projected * scale).astype(jnp.bfloat16)
    tall = min(512, clusters * depth)
    per = tall // depth
    for t in range(clusters // per):
        packed = jnp.dot(
            place[t * tall:(t + 1) * tall, :], rows[...], preferred_element_type=jnp.float32
        ).astype(jnp.bfloat16)
        some = slice(t * per, (t + 1) * per)
        send_ref[some, :depth, :] = packed[:, :LANES].reshape(per, depth, LANES)
        send_ref[some, depth:2 * depth, :] = packed[:, LANES:].reshape(per, depth, LANES)


def nearest_kernel(recv_rows, out_ref, x, col, side, *, depth):
    n, groups = recv_rows.shape[:2]
    recv_ref = recv_rows.reshape(n, groups * ROWS, LANES)
    extra = groups * ROWS - 2 * depth
    slots = n * depth
    group = LANES // depth
    x[:, :LANES] = recv_ref[:, :depth, :].reshape(slots, LANES)
    x[:, LANES:] = recv_ref[:, depth:2 * depth, :].reshape(slots, LANES)
    digit_id = lax.broadcasted_iota(jnp.int32, (n, extra, LANES), 1)
    weight = jnp.where(
        digit_id == 0, 1.0, jnp.where(digit_id == 1, float(BASE), float(BASE * BASE))
    )
    digits = recv_ref[:, 2 * depth:, :].astype(jnp.float32)
    order = jnp.sum(digits * weight, axis=1)
    lane_group = lax.broadcasted_iota(jnp.int32, (1, LANES), 1) // depth
    rows_of = []
    for k in range(slots // LANES):
        row = order[k * group:k * group + 1, :]
        for q in range(1, group):
            row = jnp.where(lane_group == q, order[k * group + q:k * group + q + 1, :], row)
        rows_of.append(row)
    turned = order.T
    for c in range(n):
        col[c * depth:(c + 1) * depth, :] = jnp.broadcast_to(
            turned[:depth, c:c + 1], (depth, LANES)
        )
    tile = 256
    tiles = slots // tile
    tops = {}
    for i in range(tiles):
        right = x[i * tile:(i + 1) * tile, :]
        best = [jnp.full((8, LANES), -1.0, jnp.float32) for _ in range(2)]
        for j in range(i + 1):
            scores = nt_dot(x[j * tile:(j + 1) * tile, :], right)
            part = slice(j * tile, (j + 1) * tile)
            here = col[part, :]
            mirrored = None
            for h in range(2):
                mine = scores[:, h * LANES:(h + 1) * LANES]
                before = here > rows_of[2 * i + h]
                kept = jnp.where(before, mine, -1.0)
                best[h] = jnp.maximum(best[h], jnp.max(kept.reshape(tile // 8, 8, LANES), axis=0))
                if j < i:
                    other = jnp.where(before, -1.0, mine)
                    mirrored = other if mirrored is None else jnp.maximum(mirrored, other)
            if j < i:
                if i > j + 1:
                    mirrored = jnp.maximum(mirrored, side[part, :])
                if i < tiles - 1:
                    side[part, :] = mirrored
                else:
                    for h in range(2):
                        turned_side = mirrored[h * LANES:(h + 1) * LANES, :].T
                        tops[2 * j + h] = jnp.maximum(
                            tops[2 * j + h], jnp.max(turned_side, axis=0, keepdims=True)
                        )
        for h in range(2):
            tops[2 * i + h] = jnp.max(best[h], axis=0, keepdims=True)
    for k in range(slots // LANES):
        for q in range(group):
            out_ref[k * group + q] = tops[k]


def collect_kernel(back_ref, cluster_ref, lane_ref, out_ref):
    n = back_ref.shape[0]
    n_rows = cluster_ref.shape[1]
    back = back_ref[...].reshape(n, LANES)
    high = back.astype(jnp.bfloat16)
    rest = back - high.astype(jnp.float32)
    middle = rest.astype(jnp.bfloat16)
    low = (rest - middle.astype(jnp.float32)).astype(jnp.bfloat16)
    hot = (
        lax.broadcasted_iota(jnp.int32, (LANES, n_rows), 0) == lane_ref[...]
    ).astype(jnp.float32).astype(jnp.bfloat16)
    parts = jnp.dot(
        jnp.concatenate([high, middle, low], axis=0), hot, preferred_element_type=jnp.float32
    )
    picked = parts[:n] + parts[n:2 * n] + parts[2 * n:]
    mine = lax.broadcasted_iota(jnp.int32, (n, n_rows), 0) == cluster_ref[...]
    out_ref[...] = jnp.sum(jnp.where(mine, picked, 0.0), axis=0, keepdims=True)


def on_device(embeddings, pca_basis, cluster, doc_index):
    n_docs = lax.axis_size("docs")
    n_rep = lax.axis_size("rep")
    n_dev = n_docs * n_rep
    doc_rows, width = embeddings.shape
    features = pca_basis.shape[1]
    clusters = CL_DEV * n_docs
    assert clusters == n_dev and features == 2 * LANES
    depth = max(2, 2 * doc_rows // clusters)
    cluster_row = cluster.reshape(1, doc_rows)
    index_row = doc_index.reshape(1, doc_rows)
    vmem = pl.BlockSpec(memory_space=pltpu.VMEM)
    hbm = pl.BlockSpec(memory_space=pltpu.HBM)
    message = 2 * depth + extra_rows(doc_rows * n_dev)

    def pack(*refs):
        project_and_pack(*refs, depth=depth, clusters=clusters, total=doc_rows * n_dev)

    send, lane = pl.pallas_call(
        pack,
        name="project_and_pack",
        compiler_params=pltpu.CompilerParams(vmem_limit_bytes=28 * 2**20),
        in_specs=[hbm, hbm, hbm, hbm],
        out_specs=[vmem, vmem],
        out_shape=[
            jax.ShapeDtypeStruct((n_dev, message // ROWS, ROWS, LANES), jnp.bfloat16),
            jax.ShapeDtypeStruct((1, doc_rows), jnp.int32),
        ],
        scratch_shapes=[
            pltpu.VMEM((1, doc_rows), jnp.int32),
            pltpu.VMEM((1, doc_rows), jnp.int32),
            pltpu.VMEM((doc_rows, width), jnp.bfloat16),
            pltpu.VMEM((width, features), jnp.bfloat16),
            pltpu.VMEM((doc_rows, features), jnp.float32),
            pltpu.VMEM((doc_rows, features), jnp.bfloat16),
            pltpu.VMEM((clusters * depth, doc_rows), jnp.bfloat16),
            pltpu.SemaphoreType.DMA((2, CHUNKS)),
            pltpu.SemaphoreType.DMA((2,)),
            pltpu.SemaphoreType.DMA((2,)),
        ],
    )(*[pltpu.with_memory_space_constraint(a, pltpu.HBM) for a in (cluster_row, index_row, embeddings, pca_basis)])
    recv = lax.all_to_all(send, OWNERS, split_axis=0, concat_axis=0, tiled=True)

    def search(*refs):
        nearest_kernel(*refs, depth=depth)

    found = pl.pallas_call(
        search,
        name="nearest",
        compiler_params=pltpu.CompilerParams(vmem_limit_bytes=16 * 2**20),
        in_specs=[vmem],
        out_specs=vmem,
        out_shape=jax.ShapeDtypeStruct((n_dev, 1, LANES), jnp.float32),
        scratch_shapes=[
            pltpu.VMEM((n_dev * depth, features), jnp.bfloat16),
            pltpu.VMEM((n_dev * depth, LANES), jnp.float32),
            pltpu.VMEM((n_dev * depth, LANES), jnp.float32),
        ],
    )(recv)
    back = lax.all_to_all(found, OWNERS, split_axis=0, concat_axis=0, tiled=True)
    nearest = pl.pallas_call(
        collect_kernel,
        name="collect",
        compiler_params=pltpu.CompilerParams(vmem_limit_bytes=8 * 2**20),
        in_specs=[vmem, vmem, vmem],
        out_specs=vmem,
        out_shape=jax.ShapeDtypeStruct((1, doc_rows), jnp.float32),
    )(back, cluster_row, lane)
    return nearest.reshape(doc_rows)


def solution(mesh):
    return jax.shard_map(
        on_device,
        mesh=mesh,
        in_specs=(P(AXES, None), P(), P(AXES, None), P(AXES)),
        out_specs=P(AXES),
        check_vma=False,
    )
```
